8 devices in a mesh: dp: 1 (over z), sp: 8 (over y, x, core).
Axes of the slice: x: 2, y: 2, z: 1, core: 2. Of those that a mesh axis runs over, the one named last changes fastest.
Arguments:
- hidden_in: bfloat16 [8, 512, 1024], P('dp', 'sp')
- positions: int32 [512], P(('dp', 'sp'))
- grad_y: bfloat16 [8, 512, 1024], P('dp', 'sp')
- w_query: bfloat16 [2, 1024, 16, 64], replicated
- w_key: bfloat16 [2, 1024, 16, 64], replicated
- w_value: bfloat16 [2, 1024, 16, 64], replicated
- w_out: bfloat16 [2, 16, 64, 1024], replicated
- w_up: bfloat16 [2, 1024, 4096], replicated
- w_down: bfloat16 [2, 4096, 1024], replicated
- gain: float32 [2, 1024], replicated
- learn_rate: float32 [], replicated
Outputs:
- output 1: bfloat16 [8, 512, 1024], P('dp', 'sp')
- output 2: bfloat16 [8, 512, 1024], P('dp', 'sp')
- output 3: bfloat16 [2, 1024, 16, 64], P('dp')
- output 4: bfloat16 [2, 1024, 16, 64], P('dp')
- output 5: bfloat16 [2, 1024, 16, 64], P('dp')
- output 6: bfloat16 [2, 16, 64, 1024], P('dp')
- output 7: bfloat16 [2, 1024, 4096], P('dp')
- output 8: bfloat16 [2, 4096, 1024], P('dp')
All inputs are finite; a program needn't handle non-finite values.
Results may differ from the reference program's by a relative error of at most 0.0114389.
Values are sent between devices in bfloat16 or wider.
A program may use at most 1 GiB of HBM per device.

```python
import jax
import jax.numpy as jnp
from jax import lax

BATCH_SIZE = 8
SEQ_LEN = 512
D_MODEL = 1024
N_HEADS = 16
KV_HEADS = 16
HEAD_DIM = 64
FF_DIM = 4096
N_LAYERS = 2

EPSILON = 1e-6
ROPE_BASE = 10000.0
NEG_LARGE = -1e30


def setup_inputs(seed: int = 0, part: int = 0) -> dict:
    base_key = jax.random.key(seed)
    part_key = jax.random.fold_in(base_key, part)
    key_noise, key_walk, key_grad, key_pos = jax.random.split(part_key, 4)
    act_shape = (BATCH_SIZE, SEQ_LEN, D_MODEL)
    noise = jax.random.normal(key_noise, act_shape, jnp.float32)
    walk = jnp.cumsum(jax.random.normal(key_walk, act_shape, jnp.float32), axis=1) * (2.0 / SEQ_LEN) ** 0.5
    steps = jax.random.randint(key_pos, (SEQ_LEN,), 1, 4, jnp.int32)
    positions = jnp.cumsum(steps) - steps[0]
    grad_y = jax.random.normal(key_grad, act_shape, jnp.float32)
    weight_keys = jax.random.split(jax.random.key(seed + 1), 8)

    def draw_weight(index, shape, fan_in):
        return (jax.random.normal(weight_keys[index], shape, jnp.float32) * fan_in ** -0.5).astype(jnp.bfloat16)

    return {
        "hidden_in": (noise + walk).astype(jnp.bfloat16),
        "positions": positions,
        "grad_y": grad_y.astype(jnp.bfloat16),
        "w_query": draw_weight(0, (N_LAYERS, D_MODEL, N_HEADS, HEAD_DIM), D_MODEL),
        "w_key": draw_weight(1, (N_LAYERS, D_MODEL, KV_HEADS, HEAD_DIM), D_MODEL),
        "w_value": draw_weight(2, (N_LAYERS, D_MODEL, KV_HEADS, HEAD_DIM), D_MODEL),
        "w_out": draw_weight(3, (N_LAYERS, N_HEADS, HEAD_DIM, D_MODEL), N_HEADS * HEAD_DIM),
        "w_up": draw_weight(4, (N_LAYERS, D_MODEL, FF_DIM), D_MODEL),
        "w_down": draw_weight(5, (N_LAYERS, FF_DIM, D_MODEL), FF_DIM),
        "gain": jax.random.uniform(weight_keys[6], (N_LAYERS, D_MODEL), jnp.float32, 0.5, 1.5),
        "learn_rate": jax.random.uniform(weight_keys[7], (), jnp.float32, 1.0, 3.0) * (BATCH_SIZE * SEQ_LEN * D_MODEL) ** -0.5,
    }


def rope_tables(positions):
    half_dim = HEAD_DIM // 2
    freqs = ROPE_BASE ** (-jnp.arange(half_dim, dtype=jnp.float32) / half_dim)
    angles = positions.astype(jnp.float32)[:, None] * freqs[None, :]
    return jnp.cos(angles)[None, :, None, :], jnp.sin(angles)[None, :, None, :]


def rotate(tensor, cos_t, sin_t):
    half_dim = tensor.shape[-1] // 2
    first = tensor[..., :half_dim]
    second = tensor[..., half_dim:]
    return jnp.concatenate([first * cos_t - second * sin_t, second * cos_t + first * sin_t], axis=-1)


def attend(queries, keys_in, values):
    groups = N_HEADS // KV_HEADS
    scale = HEAD_DIM ** -0.5
    q_blocks = queries.reshape(BATCH_SIZE, SEQ_LEN, KV_HEADS, groups, HEAD_DIM).transpose(0, 2, 3, 1, 4).reshape(BATCH_SIZE * KV_HEADS, groups, SEQ_LEN, HEAD_DIM)
    k_blocks = keys_in.transpose(0, 2, 1, 3).reshape(BATCH_SIZE * KV_HEADS, SEQ_LEN, HEAD_DIM)
    v_blocks = values.transpose(0, 2, 1, 3).reshape(BATCH_SIZE * KV_HEADS, SEQ_LEN, HEAD_DIM)
    allowed = jnp.arange(SEQ_LEN)[:, None] >= jnp.arange(SEQ_LEN)[None, :]

    def one_block(operands):
        q_one, k_one, v_one = operands
        scores = jnp.einsum("gqd,sd->gqs", q_one.astype(jnp.float32), k_one.astype(jnp.float32)) * scale
        scores = jnp.where(allowed, scores, NEG_LARGE)
        log_norm = jax.nn.logsumexp(scores, axis=-1, keepdims=True)
        probs = jnp.exp(scores - log_norm).astype(jnp.bfloat16)
        attended = jnp.einsum("gqs,sd->gqd", probs.astype(jnp.float32), v_one.astype(jnp.float32))
        return attended.astype(jnp.bfloat16)

    out_blocks = lax.map(jax.checkpoint(one_block), (q_blocks, k_blocks, v_blocks))
    return out_blocks.reshape(BATCH_SIZE, KV_HEADS, groups, SEQ_LEN, HEAD_DIM).transpose(0, 3, 1, 2, 4).reshape(BATCH_SIZE, SEQ_LEN, N_HEADS, HEAD_DIM)


def forward(hidden, w_query, w_key, w_value, w_out, w_up, w_down, gain, cos_t, sin_t):
    for layer in range(N_LAYERS):
        x_f32 = hidden.astype(jnp.float32)
        inv_rms = lax.rsqrt(jnp.mean(x_f32 * x_f32, axis=-1, keepdims=True) + EPSILON)
        normed = (x_f32 * inv_rms * gain[layer]).astype(jnp.bfloat16)
        n_f32 = normed.astype(jnp.float32)
        queries = rotate(jnp.einsum("bsd,dhe->bshe", n_f32, w_query[layer].astype(jnp.float32)), cos_t, sin_t).astype(jnp.bfloat16)
        keys_r = rotate(jnp.einsum("bsd,dhe->bshe", n_f32, w_key[layer].astype(jnp.float32)), cos_t, sin_t).astype(jnp.bfloat16)
        values = jnp.einsum("bsd,dhe->bshe", n_f32, w_value[layer].astype(jnp.float32)).astype(jnp.bfloat16)
        attended = attend(queries, keys_r, values)
        attn_part = jnp.einsum("bshe,hed->bsd", attended.astype(jnp.float32), w_out[layer].astype(jnp.float32))
        pre_act = jnp.dot(normed, w_up[layer], preferred_element_type=jnp.float32)
        act_out = jax.nn.gelu(pre_act, approximate=True).astype(jnp.bfloat16)
        mlp_part = jnp.dot(act_out, w_down[layer], preferred_element_type=jnp.float32)
        hidden = (x_f32 + attn_part + mlp_part).astype(jnp.bfloat16)
    return hidden


def reference(hidden_in, positions, grad_y, w_query, w_key, w_value, w_out, w_up, w_down, gain, learn_rate):
    cos_t, sin_t = rope_tables(positions)

    def run(hidden, query_w, key_w, value_w, out_w, up_w, down_w):
        return forward(hidden, query_w, key_w, value_w, out_w, up_w, down_w, gain, cos_t, sin_t)

    out_y, pull_back = jax.vjp(run, hidden_in, w_query, w_key, w_value, w_out, w_up, w_down)
    grads = pull_back(grad_y)
    weights = (w_query, w_key, w_value, w_out, w_up, w_down)
    updated = [(weight.astype(jnp.float32) - learn_rate * grad.astype(jnp.float32)).astype(jnp.bfloat16) for weight, grad in zip(weights, grads[1:])]
    return (out_y, grads[0], updated[0], updated[1], updated[2], updated[3], updated[4], updated[5])
```

```python
import functools
import jax
import jax.numpy as jnp
from jax import lax
from jax.experimental import pallas as pl
from jax.experimental.pallas import tpu as pltpu
from jax.sharding import PartitionSpec as P

EPSILON = 1e-6
ROPE_BASE = 10000.0
NEG_LARGE = -1e30
HD = 64
SEQ = 512
D = 1024
CB = 256
QB = 256
BF = jnp.bfloat16
F32 = jnp.float32


def norm_apply(x_f32, gain_row):
    inv_rms = lax.rsqrt(jnp.mean(x_f32 * x_f32, axis=-1, keepdims=True) + EPSILON)
    return x_f32 * inv_rms * gain_row


def dot_nn(a, b):
    return lax.dot_general(a, b, (((1,), (0,)), ((), ())), preferred_element_type=F32)


def dot_nt(a, b):
    return lax.dot_general(a, b, (((1,), (1,)), ((), ())), preferred_element_type=F32)


def swap_halves(t):
    lane = lax.broadcasted_iota(jnp.int32, t.shape, 1)
    return jnp.where(lane % HD < HD // 2, pltpu.roll(t, t.shape[1] - HD // 2, 1), pltpu.roll(t, HD // 2, 1))


def head_mask(rows, h):
    lane = lax.broadcasted_iota(jnp.int32, (rows, 128), 1)
    return lane < HD if h % 2 == 0 else lane >= HD


def causal_mask(nk, j):
    key = lax.broadcasted_iota(jnp.int32, (nk, QB), 0)
    qry = lax.broadcasted_iota(jnp.int32, (nk, QB), 1) + j * QB
    return key <= qry


def attn_fwd_kernel(n_ref, wq_ref, wk_ref, wv_ref, c_ref, s_ref, q_ref, k_ref, v_ref, o_ref, op_ref, lse_ref):
    n = n_ref[...]
    c = jnp.concatenate([c_ref[...]] * (CB // 128), axis=1)
    s = jnp.concatenate([s_ref[...]] * (CB // 128), axis=1)
    qf = dot_nn(n, wq_ref[...])
    q = (qf * c + swap_halves(qf) * s).astype(BF)
    kf = dot_nn(n, wk_ref[...])
    k = (kf * c + swap_halves(kf) * s).astype(BF)
    v = dot_nn(n, wv_ref[...]).astype(BF)
    q_ref[...] = q
    k_ref[...] = k
    v_ref[...] = v
    vt = v.T
    heads = []
    for h in range(CB // HD):
        lo = (h // 2) * 128
        qm = jnp.where(head_mask(SEQ, h), q[:, lo:lo + 128] * BF(HD ** -0.5), BF(0))
        k2 = k[:, lo:lo + 128]
        cols = []
        for j in range(SEQ // QB):
            nk = (j + 1) * QB
            st = dot_nt(k2[:nk], qm[j * QB:(j + 1) * QB])
            st = jnp.where(causal_mask(nk, j), st, NEG_LARGE)
            m = jnp.max(st, axis=0, keepdims=True)
            e = jnp.exp(st - m)
            l = jnp.sum(e, axis=0, keepdims=True)
            p = (e * (1.0 / l)).astype(BF)
            cols.append(dot_nn(vt[h * HD:(h + 1) * HD, :nk], p))
            lse_ref[h:h + 1, j * QB:(j + 1) * QB] = m + jnp.log(l)
        heads.append(jnp.concatenate(cols, axis=1))
    o = jnp.concatenate(heads, axis=0).T.astype(BF)
    o_ref[...] = o
    op_ref[0] = o[:, :128]
    op_ref[1] = o[:, 128:]


def attn_fwd(l, n, wq, wk, wv, c, s):
    nb = D // CB
    wspec = pl.BlockSpec((None, D, CB), lambda i: (l, 0, i))
    aspec = pl.BlockSpec((SEQ, CB), lambda i: (0, i))
    full = lambda shape: pl.BlockSpec(shape, lambda i: (0, 0))
    act = jax.ShapeDtypeStruct((SEQ, D), BF)
    return pl.pallas_call(
        attn_fwd_kernel,
        grid=(nb,),
        in_specs=[full((SEQ, D)), wspec, wspec, wspec, full((SEQ, 128)), full((SEQ, 128))],
        out_specs=[aspec, aspec, aspec, aspec, pl.BlockSpec((2, SEQ, 128), lambda i: (i, 0, 0)),
                   pl.BlockSpec((None, CB // HD, SEQ), lambda i: (i, 0, 0))],
        out_shape=[act, act, act, act, jax.ShapeDtypeStruct((8, SEQ, 128), BF),
                   jax.ShapeDtypeStruct((nb, CB // HD, SEQ), F32)],
        cost_estimate=pl.CostEstimate(flops=6 * SEQ * D * D + 8 * SEQ * SEQ * D, bytes_accessed=14 << 20, transcendentals=0),
        name="attn_fwd",
    )(n, wq, wk, wv, c, s)


def attn_bwd_kernel(g_ref, wo_ref, wq_ref, wk_ref, wv_ref, q_ref, k_ref, v_ref, lse_ref, c_ref, s_ref, dn_ref, dp_ref):
    do = dot_nt(g_ref[...], wo_ref[...]).astype(BF)
    q = q_ref[...]
    k = k_ref[...]
    v = v_ref[...]
    kt = k.T
    dqs, dks, dvs = [], [], []
    for h in range(CB // HD):
        lo = (h // 2) * 128
        hm = head_mask(SEQ, h)
        q2 = q[:, lo:lo + 128]
        qm = jnp.where(hm, q2 * BF(HD ** -0.5), BF(0))
        do2 = do[:, lo:lo + 128]
        dom = jnp.where(hm, do2, BF(0))
        k2 = k[:, lo:lo + 128]
        v2 = v[:, lo:lo + 128]
        dk = dv = None
        cols = []
        for j in reversed(range(SEQ // QB)):
            nk = (j + 1) * QB
            rows = slice(j * QB, (j + 1) * QB)
            st = dot_nt(k2[:nk], qm[rows])
            pt = jnp.where(causal_mask(nk, j), jnp.exp(st - lse_ref[h:h + 1, rows]), 0.0)
            dpt = dot_nt(v2[:nk], dom[rows])
            rd = jnp.sum(dpt * pt, axis=0, keepdims=True)
            dst = (pt * (dpt - rd) * HD ** -0.5).astype(BF)
            dv_j = dot_nn(pt.astype(BF), do2[rows])
            dk_j = dot_nn(dst, q2[rows])
            cols.append(dot_nn(kt[h * HD:(h + 1) * HD, :nk], dst))
            if dk is None:
                dk, dv = dk_j, dv_j
            else:
                dk = jnp.concatenate([dk[:nk] + dk_j, dk[nk:]], axis=0)
                dv = jnp.concatenate([dv[:nk] + dv_j, dv[nk:]], axis=0)
        dqs.append(jnp.concatenate(cols[::-1], axis=1))
        dks.append(dk)
        dvs.append(dv)
    c = jnp.concatenate([c_ref[...]] * (CB // 128), axis=1)
    s = jnp.concatenate([s_ref[...]] * (CB // 128), axis=1)
    low = head_mask(SEQ, 0)

    def join(parts):
        return jnp.concatenate([jnp.where(low, parts[2 * i], parts[2 * i + 1]) for i in range(CB // 128)], axis=1).astype(BF)

    def unrope(t):
        t = t.astype(F32)
        return (t * c - swap_halves(t) * s).astype(BF)

    dq = unrope(jnp.concatenate(dqs, axis=0).T.astype(BF))
    dk = unrope(join(dks))
    dv = join(dvs)
    for i in range(2):
        dp_ref[i, :, 0:128] = dq[:, i * 128:(i + 1) * 128]
        dp_ref[i, :, 128:256] = dk[:, i * 128:(i + 1) * 128]
        dp_ref[i, :, 256:384] = dv[:, i * 128:(i + 1) * 128]
    dn = dot_nt(dq, wq_ref[...]) + dot_nt(dk, wk_ref[...]) + dot_nt(dv, wv_ref[...])

    @pl.when(pl.program_id(0) == 0)
    def _():
        dn_ref[...] = dn

    @pl.when(pl.program_id(0) > 0)
    def _():
        dn_ref[...] += dn


def attn_bwd(l, g, wo, wq, wk, wv, q, k, v, lse, c, s):
    nb = D // CB
    wspec = pl.BlockSpec((None, D, CB), lambda i: (l, 0, i))
    aspec = pl.BlockSpec((SEQ, CB), lambda i: (0, i))
    full = lambda shape: pl.BlockSpec(shape, lambda i: (0, 0))
    return pl.pallas_call(
        attn_bwd_kernel,
        grid=(nb,),
        in_specs=[full((SEQ, D)), pl.BlockSpec((None, CB, D), lambda i: (l, i, 0)), wspec, wspec, wspec, aspec, aspec, aspec,
                  pl.BlockSpec((None, CB // HD, SEQ), lambda i: (i, 0, 0)), full((SEQ, 128)), full((SEQ, 128))],
        out_specs=[full((SEQ, D)), pl.BlockSpec((2, SEQ, 384), lambda i: (i, 0, 0))],
        out_shape=[jax.ShapeDtypeStruct((SEQ, D), F32), jax.ShapeDtypeStruct((8, SEQ, 384), BF)],
        cost_estimate=pl.CostEstimate(flops=8 * SEQ * D * D + 20 * SEQ * SEQ * D, bytes_accessed=20 << 20, transcendentals=0),
        name="attn_bwd",
    )(g, wo, wq, wk, wv, q, k, v, lse, c, s)


NDEV = 8
MESH_ID = pl.DeviceIdType.MESH
ANY = pl.BlockSpec(memory_space=pl.ANY)
FB = 512


class Exchange:
    def __init__(self, pairs, send_sem, recv_sem, local_sem):
        me = lax.axis_index("sp")
        self.remote, self.local = [], []
        for a, (src, dst) in enumerate(pairs):
            self.local.append(pltpu.make_async_copy(src.at[me], dst.at[me], local_sem.at[a]))
        for k in range(1, NDEV):
            peer = lax.rem(me + k, NDEV)
            for a, (src, dst) in enumerate(pairs):
                self.remote.append(pltpu.make_async_remote_copy(
                    src_ref=src.at[peer], dst_ref=dst.at[me], send_sem=send_sem.at[a, k], recv_sem=recv_sem.at[a, k],
                    device_id={"sp": peer}, device_id_type=MESH_ID))

    def start(self):
        me = lax.axis_index("sp")
        barrier = pltpu.get_barrier_semaphore()
        for k in range(1, NDEV):
            pl.semaphore_signal(barrier, inc=1, device_id={"sp": lax.rem(me + k, NDEV)}, device_id_type=MESH_ID)
        for c in self.local:
            c.start()
        pl.semaphore_wait(barrier, NDEV - 1)
        for c in self.remote:
            c.start()

    def wait(self):
        for c in self.local + self.remote:
            c.wait()


def exchange_sems(n):
    return [pltpu.SemaphoreType.DMA((n, NDEV)), pltpu.SemaphoreType.DMA((n, NDEV)), pltpu.SemaphoreType.DMA((n,))]


def entry_kernel(x_ref, p_ref, xo_ref, po_ref, ss, rs, ls):
    ex = Exchange([(x_ref, xo_ref), (p_ref, po_ref)], ss, rs, ls)
    ex.start()
    ex.wait()


def entry(x, pos):
    return pl.pallas_call(
        entry_kernel, in_specs=[ANY, ANY], out_specs=[ANY, ANY],
        out_shape=[jax.ShapeDtypeStruct(x.shape, x.dtype), jax.ShapeDtypeStruct(pos.shape, pos.dtype)],
        scratch_shapes=exchange_sems(2),
        compiler_params=pltpu.CompilerParams(collective_id=1, has_side_effects=True), name="entry",
    )(x, pos)


def gelu_parts(x):
    c = 0.7978845608028654
    x2 = x * x
    t = jnp.tanh(c * (x + 0.044715 * (x2 * x)))
    return x2, t, c


def gelu(x):
    _, t, _ = gelu_parts(x)
    return x * (0.5 * (1.0 + t))


def gelu_slope(x):
    x2, t, c = gelu_parts(x)
    return 0.5 * (1.0 + t) + 0.5 * x * (1.0 - t * t) * (c * (1.0 + 3 * 0.044715 * x2))


def mlp_fwd_kernel(last, n_ref, x_ref, o_ref, wo_ref, wu_ref, wd_ref, gain_ref, op_ref, *rest):
    if last:
        pre_ref, h_ref, oa_ref, acc_ref, ss, rs, ls = rest
    else:
        pre_ref, h_ref, oa_ref, nn_ref, acc_ref, ss, rs, ls = rest
    i = pl.program_id(0)
    ex = Exchange([(op_ref, oa_ref)], ss, rs, ls)

    @pl.when(i == 0)
    def _():
        ex.start()
        acc_ref[...] = x_ref[...].astype(F32) + dot_nn(o_ref[...], wo_ref[...])

    pre = dot_nn(n_ref[...], wu_ref[...])
    pre_ref[...] = pre
    acc_ref[...] += dot_nn(gelu(pre).astype(BF), wd_ref[...])

    @pl.when(i == pl.num_programs(0) - 1)
    def _():
        h = acc_ref[...].astype(BF)
        h_ref[...] = h
        if not last:
            nn_ref[...] = norm_apply(h.astype(F32), gain_ref[...]).astype(BF)
        ex.wait()


def mlp_fwd(l, last, n, x, o, wo, wu, wd, gain_next, o_pack):
    full = lambda shape: pl.BlockSpec(shape, lambda i: (0, 0))
    ff = wu.shape[2]
    act = jax.ShapeDtypeStruct((SEQ, D), BF)
    out_specs = [pl.BlockSpec((SEQ, FB), lambda i: (0, i)), full((SEQ, D)), ANY]
    out_shape = [jax.ShapeDtypeStruct((SEQ, ff), F32), act, jax.ShapeDtypeStruct(o_pack.shape, BF)]
    if not last:
        out_specs.append(full((SEQ, D)))
        out_shape.append(act)
    return pl.pallas_call(
        functools.partial(mlp_fwd_kernel, last), grid=(ff // FB,),
        in_specs=[full((SEQ, D)), full((SEQ, D)), full((SEQ, D)), pl.BlockSpec((None, D, D), lambda i: (l, 0, 0)),
                  pl.BlockSpec((None, D, FB), lambda i: (l, 0, i)), pl.BlockSpec((None, FB, D), lambda i: (l, i, 0)),
                  full((1, D)), ANY],
        out_specs=out_specs, out_shape=out_shape,
        scratch_shapes=[pltpu.VMEM((SEQ, D), F32)] + exchange_sems(1),
        compiler_params=pltpu.CompilerParams(collective_id=2 + l, has_side_effects=True),
        cost_estimate=pl.CostEstimate(flops=4 * SEQ * D * ff + 2 * SEQ * D * D, bytes_accessed=30 << 20, transcendentals=0),
        name="mlp_fwd",
    )(n, x, o, wo, wu, wd, gain_next, o_pack)


def mlp_bwd_kernel(g_ref, pre_ref, wu_ref, wd_ref, dn_ref, x_ref, gain_ref, go_ref, acc_ref):
    i = pl.program_id(0)

    @pl.when(i == 0)
    def _():
        acc_ref[...] = dn_ref[...]

    d_act = dot_nt(g_ref[...], wd_ref[...]).astype(BF)
    d_pre = (d_act.astype(F32) * gelu_slope(pre_ref[...])).astype(BF)
    acc_ref[...] += dot_nt(d_pre, wu_ref[...])

    @pl.when(i == pl.num_programs(0) - 1)
    def _():
        x = x_ref[...].astype(F32)
        r = lax.rsqrt(jnp.mean(x * x, axis=-1, keepdims=True) + EPSILON)
        t = acc_ref[...] * gain_ref[...]
        dot = jnp.mean(x * t, axis=-1, keepdims=True)
        dx = r * t - x * (r * r * r * dot)
        go_ref[...] = (g_ref[...].astype(F32) + dx).astype(BF)


def mlp_bwd(l, g, pre, wu, wd, dn, x, gain_row):
    full = lambda shape: pl.BlockSpec(shape, lambda i: (0, 0))
    ff = wu.shape[2]
    return pl.pallas_call(
        mlp_bwd_kernel, grid=(ff // FB,),
        in_specs=[full((SEQ, D)), pl.BlockSpec((SEQ, FB), lambda i: (0, i)), pl.BlockSpec((None, D, FB), lambda i: (l, 0, i)),
                  pl.BlockSpec((None, FB, D), lambda i: (l, i, 0)), full((SEQ, D)), full((SEQ, D)), full((1, D))],
        out_specs=full((SEQ, D)), out_shape=jax.ShapeDtypeStruct((SEQ, D), BF),
        scratch_shapes=[pltpu.VMEM((SEQ, D), F32)],
        cost_estimate=pl.CostEstimate(flops=4 * SEQ * D * ff, bytes_accessed=30 << 20, transcendentals=0),
        name="mlp_bwd",
    )(g, pre, wu, wd, dn, x, gain_row)


def dw_mlp_kernel(lr_ref, n_ref, g_ref, wu_ref, wd_ref, dp_ref, sq_ref, w_ref, da_ref, so_ref, wut_ref, au_ref, ad_ref, ss, rs, ls):
    i = pl.program_id(0)
    ex = Exchange([(dp_ref, da_ref), (sq_ref, so_ref)], ss, rs, ls)

    @pl.when(i == 0)
    def _():
        ex.start()
        wut_ref[...] = wu_ref[...].T
        au_ref[...] = jnp.zeros_like(au_ref)
        ad_ref[...] = jnp.zeros_like(ad_ref)

    n = n_ref[...]
    g = g_ref[...].reshape(SEQ, D)
    pre = dot_nt(wut_ref[...], n)
    d_act = dot_nt(wd_ref[...], g).astype(BF)
    x2, t, c = gelu_parts(pre)
    half = 0.5 * (1.0 + t)
    act = (pre * half).astype(BF)
    slope = half + 0.5 * pre * (1.0 - t * t) * (c * (1.0 + 3 * 0.044715 * x2))
    d_pre = (d_act.astype(F32) * slope).astype(BF)
    ad_ref[...] += dot_nn(act, g)
    au_ref[...] += dot_nn(d_pre, n)

    @pl.when(i == pl.num_programs(0) - 1)
    def _():
        lr = lr_ref[0]
        w_ref[0:D] = (wut_ref[...].astype(F32) - lr * au_ref[...]).astype(BF).T
        nd = (wd_ref[...].astype(F32) - lr * ad_ref[...]).astype(BF)
        w_ref[D:D + FB] = nd[:, :FB]
        w_ref[D + FB:] = nd[:, FB:]
        ex.wait()


def dw_mlp(l, lr, n_all, g4, wu_s, wd_s, d_pack, seq_out):
    full = lambda shape: pl.BlockSpec(shape, lambda i: (0, 0))
    gs = g4.shape
    return pl.pallas_call(
        dw_mlp_kernel, grid=(NDEV,),
        in_specs=[pl.BlockSpec(memory_space=pltpu.SMEM), pl.BlockSpec((SEQ, D), lambda i: (i, 0)),
                  pl.BlockSpec((gs[0], None, gs[2], D), lambda i: (0, i, 0, 0)), full((D, FB)), full((FB, D)), ANY, ANY],
        out_specs=[full((2 * D, FB)), ANY, ANY],
        out_shape=[jax.ShapeDtypeStruct((2 * D, FB), BF), jax.ShapeDtypeStruct(d_pack.shape, BF),
                   jax.ShapeDtypeStruct(seq_out.shape, BF)],
        scratch_shapes=[pltpu.VMEM((FB, D), BF), pltpu.VMEM((FB, D), F32), pltpu.VMEM((FB, D), F32)] + exchange_sems(2),
        compiler_params=pltpu.CompilerParams(collective_id=4 + l, has_side_effects=True),
        cost_estimate=pl.CostEstimate(flops=8 * NDEV * SEQ * D * FB, bytes_accessed=24 << 20, transcendentals=0),
        name="dw_mlp",
    )(lr, n_all, g4, wu_s, wd_s, d_pack, seq_out)


def dw_attn_kernel(lr_ref, n_ref, g_ref, d_ref, o_ref, wqkv_ref, wo_ref, w_ref, aq_ref, ao_ref):
    i = pl.program_id(0)

    @pl.when(i == 0)
    def _():
        aq_ref[...] = jnp.zeros_like(aq_ref)
        ao_ref[...] = jnp.zeros_like(ao_ref)

    aq_ref[...] += dot_nn(d_ref[...].T, n_ref[...])
    ao_ref[...] += dot_nn(o_ref[...].T, g_ref[...].reshape(SEQ, D))

    @pl.when(i == pl.num_programs(0) - 1)
    def _():
        lr = lr_ref[0]
        w_ref[:, 0:384] = (wqkv_ref[...].astype(F32) - lr * aq_ref[...].T).astype(BF)
        no = (wo_ref[...].astype(F32) - lr * ao_ref[...]).astype(BF)
        for c in range(D // 128):
            w_ref[c * 128:(c + 1) * 128, 384:512] = no[:, c * 128:(c + 1) * 128]


def dw_attn(lr, n_all, g4, d_all, o_all, wqkv_s, wo_s):
    full = lambda shape: pl.BlockSpec(shape, lambda i: (0, 0))
    gs = g4.shape
    return pl.pallas_call(
        dw_attn_kernel, grid=(NDEV,),
        in_specs=[pl.BlockSpec(memory_space=pltpu.SMEM), pl.BlockSpec((SEQ, D), lambda i: (i, 0)),
                  pl.BlockSpec((gs[0], None, gs[2], D), lambda i: (0, i, 0, 0)),
                  pl.BlockSpec((None, SEQ, 384), lambda i: (i, 0, 0)), pl.BlockSpec((None, SEQ, 128), lambda i: (i, 0, 0)),
                  full((D, 384)), full((128, D))],
        out_specs=full((D, 512)), out_shape=jax.ShapeDtypeStruct((D, 512), BF),
        scratch_shapes=[pltpu.VMEM((384, D), F32), pltpu.VMEM((128, D), F32)],
        cost_estimate=pl.CostEstimate(flops=2 * NDEV * SEQ * D * 512, bytes_accessed=24 << 20, transcendentals=0),
        name="dw_attn",
    )(lr, n_all, g4, d_all, o_all, wqkv_s, wo_s)


def place_mlp_kernel(w_ref, *rest):
    u_ref, d_ref = rest[-2:]
    u_ref[...] = w_ref[0:D]
    d_ref[:, :FB] = w_ref[D:D + FB]
    d_ref[:, FB:] = w_ref[D + FB:]


def place_mlp(l, layers, w_all, prev):
    prev = list(prev)
    ff = NDEV * FB
    return pl.pallas_call(
        place_mlp_kernel, grid=(NDEV,),
        in_specs=[pl.BlockSpec((2 * D, FB), lambda i: (i, 0))] + [ANY] * len(prev),
        out_specs=[pl.BlockSpec((None, D, FB), lambda i: (l, 0, i)), pl.BlockSpec((None, FB, D), lambda i: (l, i, 0))],
        out_shape=[jax.ShapeDtypeStruct((layers, D, ff), BF), jax.ShapeDtypeStruct((layers, ff, D), BF)],
        input_output_aliases={1 + i: i for i in range(len(prev))},
        cost_estimate=pl.CostEstimate(flops=1 << 30, bytes_accessed=32 << 20, transcendentals=0),
        name="place_mlp",
    )(w_all, *prev)


def place_attn_kernel(w_ref, *rest):
    q_ref, k_ref, v_ref, o_ref = rest[-4:]
    q_ref[...] = w_ref[:, 0:128]
    k_ref[...] = w_ref[:, 128:256]
    v_ref[...] = w_ref[:, 256:384]
    for c in range(D // 128):
        o_ref[:, c * 128:(c + 1) * 128] = w_ref[c * 128:(c + 1) * 128, 384:512]


def place_attn(l, layers, w_all, prev):
    prev = list(prev)
    col = pl.BlockSpec((None, D, 128), lambda i: (l, 0, i))
    return pl.pallas_call(
        place_attn_kernel, grid=(NDEV,),
        in_specs=[pl.BlockSpec((D, 512), lambda i: (i, 0))] + [ANY] * len(prev),
        out_specs=[col, col, col, pl.BlockSpec((None, 128, D), lambda i: (l, i, 0))],
        out_shape=[jax.ShapeDtypeStruct((layers, D, D), BF)] * 4,
        input_output_aliases={1 + i: i for i in range(len(prev))},
        cost_estimate=pl.CostEstimate(flops=1 << 30, bytes_accessed=16 << 20, transcendentals=0),
        name="place_attn",
    )(w_all, *prev)


def solution(mesh):
    act_spec = P("dp", "sp", None)
    out_four = P("dp", None, None, None)
    out_three = P("dp", None, None)

    def step(hidden_in, positions, grad_y, w_query, w_key, w_value, w_out, w_up, w_down, gain, learn_rate):
        layers = w_query.shape[0]
        idx = lax.axis_index("sp")
        chunk = SEQ // NDEV
        lr = learn_rate.reshape(1)

        def gather(t):
            return lax.all_gather(t, "sp", axis=0, tiled=True)

        gy_all = lax.all_gather(grad_y, "sp", axis=0, tiled=False)
        pos_tile = jnp.zeros((8, 128), jnp.int32).at[0, :chunk].set(positions)
        x_in, pos_all = entry(hidden_in, jnp.broadcast_to(pos_tile, (NDEV, 8, 128)))
        pos = pos_all[:, 0, :chunk].reshape(SEQ)
        lane = jnp.arange(128, dtype=jnp.int32)
        freqs = ROPE_BASE ** (-(lane % (HD // 2)).astype(F32) / (HD // 2))
        angles = pos.astype(F32)[:, None] * freqs[None, :]
        c_tab = jnp.cos(angles)
        s_tab = jnp.sin(angles) * jnp.where(lane % HD < HD // 2, -1.0, 1.0)[None, :]

        wq = w_query.reshape(layers, D, D)
        wk = w_key.reshape(layers, D, D)
        wv = w_value.reshape(layers, D, D)
        wo = w_out.reshape(layers, D, D)

        saved = []
        hidden = x_in.reshape(SEQ, D)
        normed = norm_apply(hidden.astype(F32), gain[0]).astype(BF)
        for l in range(layers):
            last = l == layers - 1
            q, k, v, o, o_pack, lse = attn_fwd(l, normed, wq, wk, wv, c_tab, s_tab)
            gain_next = gain[min(l + 1, layers - 1)].reshape(1, D)
            out = mlp_fwd(l, last, normed, hidden, o, wo, w_up, w_down, gain_next, o_pack)
            saved.append((hidden, gather(normed), q, k, v, lse, out[2], out[0]))
            hidden = out[1]
            if not last:
                normed = out[3]
        seq_out = hidden.reshape(NDEV, chunk, D)

        grad_h = lax.dynamic_index_in_dim(gy_all, idx, 1, keepdims=False).reshape(SEQ, D)
        g4 = gy_all
        mlp_new, attn_new, seq_res = (), (), []
        for l in reversed(range(layers)):
            hidden_prev, n_all, q, k, v, lse, o_all, pre = saved[l]
            dn_attn, d_pack = attn_bwd(l, grad_h, wo, wq, wk, wv, q, k, v, lse, c_tab, s_tab)
            grad_h = mlp_bwd(l, grad_h, pre, w_up, w_down, dn_attn, hidden_prev, gain[l].reshape(1, D))
            if l > 0:
                g_next = gather(grad_h).reshape(1, NDEV, SEQ, D)
            else:
                seq_out = grad_h.reshape(NDEV, chunk, D)
            wu_s = lax.dynamic_slice(w_up, (l, 0, idx * FB), (1, D, FB))[0]
            wd_s = lax.dynamic_slice(w_down, (l, idx * FB, 0), (1, FB, D))[0]
            wqkv_s = jnp.concatenate([lax.dynamic_slice(w, (l, 0, idx * 128), (1, D, 128))[0] for w in (wq, wk, wv)], axis=1)
            wo_s = lax.dynamic_slice(wo, (l, idx * 128, 0), (1, 128, D))[0]
            w_mlp, d_all, seq_in = dw_mlp(l, lr, n_all, g4, wu_s, wd_s, d_pack, seq_out)
            seq_res.append(seq_in)
            w_attn = dw_attn(lr, n_all, g4, d_all, o_all, wqkv_s, wo_s)
            mlp_new = place_mlp(l, layers, gather(w_mlp), mlp_new)
            attn_new = place_attn(l, layers, gather(w_attn), attn_new)
            if l > 0:
                g4 = g_next
        out_y, grad_x = seq_res[0], seq_res[-1]
        nq, nk, nv, no = attn_new
        return (out_y, grad_x, nq.reshape(w_query.shape), nk.reshape(w_query.shape), nv.reshape(w_query.shape),
                no.reshape(w_out.shape), mlp_new[0], mlp_new[1])

    return jax.shard_map(step, mesh=mesh,
                         in_specs=(act_spec, P(("dp", "sp")), act_spec, P(), P(), P(), P(), P(), P(), P(), P()),
                         out_specs=(act_spec, act_spec, out_four, out_four, out_four, out_four, out_three, out_three),
                         check_vma=False)
```

```python
import functools
import jax
import jax.numpy as jnp
from jax import lax
from jax.experimental import pallas as pl
from jax.experimental.pallas import tpu as pltpu
from jax.sharding import PartitionSpec as P

EPSILON = 1e-6
ROPE_BASE = 10000.0
NEG_LARGE = -1e30
HD = 64
SEQ = 512
LANE = 128
QKV = 384
D = 1024
CB = 256
QB = 256
BF = jnp.bfloat16
F32 = jnp.float32


ANY = pl.BlockSpec(memory_space=pl.ANY)
SMEM = pl.BlockSpec(memory_space=pltpu.SMEM)


def full(*shape):
    return pl.BlockSpec(shape, lambda i: (0, 0))


def cost(flops, mib):
    return pl.CostEstimate(flops=flops, bytes_accessed=mib << 20, transcendentals=0)


def norm_apply(x_f32, gain_row):
    inv_rms = lax.rsqrt(jnp.mean(x_f32 * x_f32, axis=-1, keepdims=True) + EPSILON)
    return x_f32 * inv_rms * gain_row


def dot_nn(a, b):
    return lax.dot_general(a, b, (((1,), (0,)), ((), ())), preferred_element_type=F32)


def dot_nt(a, b):
    return lax.dot_general(a, b, (((1,), (1,)), ((), ())), preferred_element_type=F32)


def swap_halves(t):
    lane = lax.broadcasted_iota(jnp.int32, t.shape, 1)
    return jnp.where(lane % HD < HD // 2, pltpu.roll(t, t.shape[1] - HD // 2, 1), pltpu.roll(t, HD // 2, 1))


def head_mask(rows, h):
    lane = lax.broadcasted_iota(jnp.int32, (rows, LANE), 1)
    return lane < HD if h % 2 == 0 else lane >= HD


def causal_mask(nk, j):
    key = lax.broadcasted_iota(jnp.int32, (nk, QB), 0)
    qry = lax.broadcasted_iota(jnp.int32, (nk, QB), 1) + j * QB
    return key <= qry


def attn_fwd_kernel(n_ref, wq_ref, wk_ref, wv_ref, c_ref, s_ref, q_ref, k_ref, v_ref, o_ref, op_ref, lse_ref):
    n = n_ref[...]
    c = jnp.concatenate([c_ref[...]] * (CB // LANE), axis=1)
    s = jnp.concatenate([s_ref[...]] * (CB // LANE), axis=1)
    qf = dot_nn(n, wq_ref[...])
    q = (qf * c + swap_halves(qf) * s).astype(BF)
    kf = dot_nn(n, wk_ref[...])
    k = (kf * c + swap_halves(kf) * s).astype(BF)
    v = dot_nn(n, wv_ref[...]).astype(BF)
    q_ref[...] = q
    k_ref[...] = k
    v_ref[...] = v
    vt = v.T
    heads = []
    for h in range(CB // HD):
        lo = (h // 2) * LANE
        qm = jnp.where(head_mask(SEQ, h), q[:, lo:lo + LANE] * BF(HD ** -0.5), BF(0))
        k2 = k[:, lo:lo + LANE]
        cols = []
        for j in range(SEQ // QB):
            nk = (j + 1) * QB
            st = dot_nt(k2[:nk], qm[j * QB:(j + 1) * QB])
            st = jnp.where(causal_mask(nk, j), st, NEG_LARGE)
            m = jnp.max(st, axis=0, keepdims=True)
            e = jnp.exp(st - m)
            l = jnp.sum(e, axis=0, keepdims=True)
            p = (e * (1.0 / l)).astype(BF)
            cols.append(dot_nn(vt[h * HD:(h + 1) * HD, :nk], p))
            lse_ref[h:h + 1, j * QB:(j + 1) * QB] = m + jnp.log(l)
        heads.append(jnp.concatenate(cols, axis=1))
    o = jnp.concatenate(heads, axis=0).T.astype(BF)
    o_ref[...] = o
    op_ref[0] = o[:, :LANE]
    op_ref[1] = o[:, LANE:]


def attn_fwd(l, n, wq, wk, wv, c, s):
    nb = D // CB
    wspec = pl.BlockSpec((None, D, CB), lambda i: (l, 0, i))
    aspec = pl.BlockSpec((SEQ, CB), lambda i: (0, i))
    act = jax.ShapeDtypeStruct((SEQ, D), BF)
    return pl.pallas_call(
        attn_fwd_kernel,
        grid=(nb,),
        in_specs=[full(SEQ, D), wspec, wspec, wspec, full(SEQ, LANE), full(SEQ, LANE)],
        out_specs=[aspec, aspec, aspec, aspec, pl.BlockSpec((2, SEQ, LANE), lambda i: (i, 0, 0)),
                   pl.BlockSpec((None, CB // HD, SEQ), lambda i: (i, 0, 0))],
        out_shape=[act, act, act, act, jax.ShapeDtypeStruct((8, SEQ, LANE), BF),
                   jax.ShapeDtypeStruct((nb, CB // HD, SEQ), F32)],
        cost_estimate=cost(6 * SEQ * D * D + 8 * SEQ * SEQ * D, 14),
        name="attn_fwd",
    )(n, wq, wk, wv, c, s)


def attn_bwd_kernel(g_ref, wo_ref, wq_ref, wk_ref, wv_ref, q_ref, k_ref, v_ref, lse_ref, c_ref, s_ref, dn_ref, dp_ref):
    do = dot_nt(g_ref[...], wo_ref[...]).astype(BF)
    q = q_ref[...]
    k = k_ref[...]
    v = v_ref[...]
    kt = k.T
    dqs, dks, dvs = [], [], []
    for h in range(CB // HD):
        lo = (h // 2) * LANE
        hm = head_mask(SEQ, h)
        q2 = q[:, lo:lo + LANE]
        qm = jnp.where(hm, q2 * BF(HD ** -0.5), BF(0))
        do2 = do[:, lo:lo + LANE]
        dom = jnp.where(hm, do2, BF(0))
        k2 = k[:, lo:lo + LANE]
        v2 = v[:, lo:lo + LANE]
        dk = dv = None
        cols = []
        for j in reversed(range(SEQ // QB)):
            nk = (j + 1) * QB
            rows = slice(j * QB, (j + 1) * QB)
            st = dot_nt(k2[:nk], qm[rows])
            pt = jnp.where(causal_mask(nk, j), jnp.exp(st - lse_ref[h:h + 1, rows]), 0.0)
            dpt = dot_nt(v2[:nk], dom[rows])
            rd = jnp.sum(dpt * pt, axis=0, keepdims=True)
            dst = (pt * (dpt - rd) * HD ** -0.5).astype(BF)
            dv_j = dot_nn(pt.astype(BF), do2[rows])
            dk_j = dot_nn(dst, q2[rows])
            cols.append(dot_nn(kt[h * HD:(h + 1) * HD, :nk], dst))
            if dk is None:
                dk, dv = dk_j, dv_j
            else:
                dk = jnp.concatenate([dk[:nk] + dk_j, dk[nk:]], axis=0)
                dv = jnp.concatenate([dv[:nk] + dv_j, dv[nk:]], axis=0)
        dqs.append(jnp.concatenate(cols[::-1], axis=1))
        dks.append(dk)
        dvs.append(dv)
    c = jnp.concatenate([c_ref[...]] * (CB // LANE), axis=1)
    s = jnp.concatenate([s_ref[...]] * (CB // LANE), axis=1)
    low = head_mask(SEQ, 0)

    def join(parts):
        return jnp.concatenate([jnp.where(low, parts[2 * i], parts[2 * i + 1]) for i in range(CB // LANE)], axis=1).astype(BF)

    def unrope(t):
        t = t.astype(F32)
        return (t * c - swap_halves(t) * s).astype(BF)

    dq = unrope(jnp.concatenate(dqs, axis=0).T.astype(BF))
    dk = unrope(join(dks))
    dv = join(dvs)
    for i in range(2):
        dp_ref[i, :, 0:LANE] = dq[:, i * LANE:(i + 1) * LANE]
        dp_ref[i, :, LANE:256] = dk[:, i * LANE:(i + 1) * LANE]
        dp_ref[i, :, 256:QKV] = dv[:, i * LANE:(i + 1) * LANE]
    dn = dot_nt(dq, wq_ref[...]) + dot_nt(dk, wk_ref[...]) + dot_nt(dv, wv_ref[...])

    @pl.when(pl.program_id(0) == 0)
    def _():
        dn_ref[...] = dn

    @pl.when(pl.program_id(0) > 0)
    def _():
        dn_ref[...] += dn


def attn_bwd(l, g, wo, wq, wk, wv, q, k, v, lse, c, s):
    nb = D // CB
    wspec = pl.BlockSpec((None, D, CB), lambda i: (l, 0, i))
    aspec = pl.BlockSpec((SEQ, CB), lambda i: (0, i))
    return pl.pallas_call(
        attn_bwd_kernel,
        grid=(nb,),
        in_specs=[full(SEQ, D), pl.BlockSpec((None, CB, D), lambda i: (l, i, 0)), wspec, wspec, wspec, aspec, aspec, aspec,
                  pl.BlockSpec((None, CB // HD, SEQ), lambda i: (i, 0, 0)), full(SEQ, LANE), full(SEQ, LANE)],
        out_specs=[full(SEQ, D), pl.BlockSpec((2, SEQ, QKV), lambda i: (i, 0, 0))],
        out_shape=[jax.ShapeDtypeStruct((SEQ, D), F32), jax.ShapeDtypeStruct((8, SEQ, QKV), BF)],
        cost_estimate=cost(8 * SEQ * D * D + 20 * SEQ * SEQ * D, 20),
        name="attn_bwd",
    )(g, wo, wq, wk, wv, q, k, v, lse, c, s)


NDEV = 8
MB = 1024
MESH_ID = pl.DeviceIdType.MESH
FB = 512


def token_spec(t, tile=lambda i: i):
    return pl.BlockSpec((t.shape[0], None, t.shape[2], D), lambda i: (0, tile(i), 0, 0))


class Exchange:
    def __init__(self, pairs, send_sem, recv_sem, local_sem):
        me = lax.axis_index("sp")
        self.remote, self.local = [], []
        for a, (src, dst) in enumerate(pairs):
            self.local.append(pltpu.make_async_copy(src.at[me], dst.at[me], local_sem.at[a]))
        for k in range(1, NDEV):
            peer = lax.rem(me + k, NDEV)
            for a, (src, dst) in enumerate(pairs):
                self.remote.append(pltpu.make_async_remote_copy(
                    src_ref=src.at[peer], dst_ref=dst.at[me], send_sem=send_sem.at[a, k], recv_sem=recv_sem.at[a, k],
                    device_id={"sp": peer}, device_id_type=MESH_ID))

    def start(self):
        me = lax.axis_index("sp")
        barrier = pltpu.get_barrier_semaphore()
        for k in range(1, NDEV):
            pl.semaphore_signal(barrier, inc=1, device_id={"sp": lax.rem(me + k, NDEV)}, device_id_type=MESH_ID)
        for c in self.local:
            c.start()
        pl.semaphore_wait(barrier, NDEV - 1)
        for c in self.remote:
            c.start()

    def wait(self):
        for c in self.local + self.remote:
            c.wait()


def exchange_sems(n):
    return [pltpu.SemaphoreType.DMA((n, NDEV)), pltpu.SemaphoreType.DMA((n, NDEV)), pltpu.SemaphoreType.DMA((n,))]


def share_kernel(p_ref, po_ref, ss, rs, ls):
    ex = Exchange([(p_ref, po_ref)], ss, rs, ls)
    ex.start()
    ex.wait()


def share(pos):
    return pl.pallas_call(
        share_kernel, in_specs=[ANY], out_specs=ANY, out_shape=jax.ShapeDtypeStruct(pos.shape, pos.dtype),
        scratch_shapes=exchange_sems(1),
        compiler_params=pltpu.CompilerParams(collective_id=1, has_side_effects=True), name="share",
    )(pos)


def gelu_parts(x):
    c = 0.7978845608028654
    x2 = x * x
    t = jnp.tanh(c * (x + 0.044715 * (x2 * x)))
    return x2, t, c


def gelu(x):
    _, t, _ = gelu_parts(x)
    return x * (0.5 * (1.0 + t))


def gelu_slope(x):
    x2, t, c = gelu_parts(x)
    return 0.5 * (1.0 + t) + 0.5 * x * (1.0 - t * t) * (c * (1.0 + 3 * 0.044715 * x2))


def mlp_fwd_kernel(last, n_ref, x_ref, o_ref, wo_ref, wu_ref, wd_ref, gain_ref, *rest):
    if last:
        pre_ref, h_ref, acc_ref = rest
    else:
        pre_ref, h_ref, nn_ref, acc_ref = rest
    i = pl.program_id(0)

    @pl.when(i == 0)
    def _():
        acc_ref[...] = x_ref[...].astype(F32) + dot_nn(o_ref[...], wo_ref[...])

    pre = dot_nn(n_ref[...], wu_ref[...])
    pre_ref[...] = pre
    acc_ref[...] += dot_nn(gelu(pre).astype(BF), wd_ref[...])

    @pl.when(i == pl.num_programs(0) - 1)
    def _():
        h = acc_ref[...].astype(BF)
        h_ref[...] = h
        if not last:
            nn_ref[...] = norm_apply(h.astype(F32), gain_ref[...]).astype(BF)


def mlp_fwd(l, last, n, x, o, wo, wu, wd, gain_next):
    ff = wu.shape[2]
    act = jax.ShapeDtypeStruct((SEQ, D), BF)
    out_specs = [pl.BlockSpec((SEQ, MB), lambda i: (0, i)), full(SEQ, D)]
    out_shape = [jax.ShapeDtypeStruct((SEQ, ff), F32), act]
    if not last:
        out_specs.append(full(SEQ, D))
        out_shape.append(act)
    return pl.pallas_call(
        functools.partial(mlp_fwd_kernel, last), grid=(ff // MB,),
        in_specs=[full(SEQ, D), full(SEQ, D), full(SEQ, D), pl.BlockSpec((None, D, D), lambda i: (l, 0, 0)),
                  pl.BlockSpec((None, D, MB), lambda i: (l, 0, i)), pl.BlockSpec((None, MB, D), lambda i: (l, i, 0)),
                  full(1, D)],
        out_specs=out_specs, out_shape=out_shape,
        scratch_shapes=[pltpu.VMEM((SEQ, D), F32)],
        cost_estimate=cost(4 * SEQ * D * ff + 2 * SEQ * D * D, 30),
        name="mlp_fwd",
    )(n, x, o, wo, wu, wd, gain_next)


def mlp_bwd_kernel(g_ref, pre_ref, wu_ref, wd_ref, dn_ref, x_ref, gain_ref, go_ref, acc_ref):
    i = pl.program_id(0)

    @pl.when(i == 0)
    def _():
        acc_ref[...] = dn_ref[...]

    d_act = dot_nt(g_ref[...], wd_ref[...]).astype(BF)
    d_pre = (d_act.astype(F32) * gelu_slope(pre_ref[...])).astype(BF)
    acc_ref[...] += dot_nt(d_pre, wu_ref[...])

    @pl.when(i == pl.num_programs(0) - 1)
    def _():
        x = x_ref[...].astype(F32)
        r = lax.rsqrt(jnp.mean(x * x, axis=-1, keepdims=True) + EPSILON)
        t = acc_ref[...] * gain_ref[...]
        dot = jnp.mean(x * t, axis=-1, keepdims=True)
        dx = r * t - x * (r * r * r * dot)
        go_ref[...] = (g_ref[...].astype(F32) + dx).astype(BF)


def mlp_bwd(l, g, pre, wu, wd, dn, x, gain_row):
    ff = wu.shape[2]
    return pl.pallas_call(
        mlp_bwd_kernel, grid=(ff // MB,),
        in_specs=[full(SEQ, D), pl.BlockSpec((SEQ, MB), lambda i: (0, i)), pl.BlockSpec((None, D, MB), lambda i: (l, 0, i)),
                  pl.BlockSpec((None, MB, D), lambda i: (l, i, 0)), full(SEQ, D), full(SEQ, D), full(1, D)],
        out_specs=full(SEQ, D), out_shape=jax.ShapeDtypeStruct((SEQ, D), BF),
        scratch_shapes=[pltpu.VMEM((SEQ, D), F32)],
        cost_estimate=cost(4 * SEQ * D * ff, 30),
        name="mlp_bwd",
    )(g, pre, wu, wd, dn, x, gain_row)


def dw_tile(wut, wd, n, g, au_ref, ad_ref):
    pre = dot_nt(wut, n)
    d_act = dot_nt(wd, g).astype(BF)
    x2, t, c = gelu_parts(pre)
    half = 0.5 * (1.0 + t)
    act = (pre * half).astype(BF)
    slope = half + 0.5 * pre * (1.0 - t * t) * (c * (1.0 + 3 * 0.044715 * x2))
    d_pre = (d_act.astype(F32) * slope).astype(BF)
    ad_ref[...] += dot_nn(act, g)
    au_ref[...] += dot_nn(d_pre, n)


def dw_finish(lr, wut, wd, au, ad):
    nu = (wut.astype(F32) - lr * au).astype(BF).T
    nd = (wd.astype(F32) - lr * ad).astype(BF)
    return nu, nd


def load_block(l, col, wu_ref, wd_ref, wu_buf, wd_buf, sem):
    at = pl.ds(pl.multiple_of(col * FB, FB), FB)
    return (pltpu.make_async_copy(wu_ref.at[l, :, at], wu_buf, sem.at[0]),
            pltpu.make_async_copy(wd_ref.at[l, at, :], wd_buf, sem.at[1]))


def dw_start(block, wu, wut_ref, au_ref, ad_ref):
    for c in block:
        c.wait()
    wut_ref[...] = wu[...].T
    au_ref[...] = jnp.zeros_like(au_ref)
    ad_ref[...] = jnp.zeros_like(ad_ref)


def dw_mlp_kernel(l, lr_ref, n_ref, g_ref, wu_ref, wd_ref, nu_ref, nd_ref, wut_ref, au_ref, ad_ref, wu_buf, wd_buf, sem):
    i = pl.program_id(0)

    @pl.when(i == 0)
    def _():
        block = load_block(l, lax.axis_index("sp"), wu_ref, wd_ref, wu_buf, wd_buf, sem)
        for c in block:
            c.start()
        dw_start(block, wu_buf, wut_ref, au_ref, ad_ref)

    dw_tile(wut_ref[...], wd_buf[...], n_ref[...].reshape(SEQ, D), g_ref[...].reshape(SEQ, D), au_ref, ad_ref)

    @pl.when(i == pl.num_programs(0) - 1)
    def _():
        nu_ref[...], nd_ref[...] = dw_finish(lr_ref[0], wut_ref[...], wd_buf[...], au_ref[...], ad_ref[...])


def dw_mlp(l, lr, n_all, g4, wu, wd):
    return pl.pallas_call(
        functools.partial(dw_mlp_kernel, l), grid=(NDEV,),
        in_specs=[SMEM, token_spec(n_all), token_spec(g4), ANY, ANY],
        out_specs=[full(D, FB), full(FB, D)], out_shape=[jax.ShapeDtypeStruct((D, FB), BF), jax.ShapeDtypeStruct((FB, D), BF)],
        scratch_shapes=[pltpu.VMEM((FB, D), BF), pltpu.VMEM((FB, D), F32), pltpu.VMEM((FB, D), F32),
                        pltpu.VMEM((D, FB), BF), pltpu.VMEM((FB, D), BF), pltpu.SemaphoreType.DMA((2,))],
        cost_estimate=cost(8 * NDEV * SEQ * D * FB, 24),
        name="dw_mlp",
    )(lr, n_all, g4, wu, wd)


NB = 2


def dw_chip_kernel(part, lr_ref, n_ref, g_ref, wu_ref, wd_ref, src_ref, st_ref, all_ref, wut_ref, au_ref, ad_ref, buf_ref,
                   wu_buf, wd_buf, st_s, st_r, st_l, sem, sp_s, sp_r):
    s = pl.program_id(0)
    me = lax.axis_index("sp")
    core = lax.rem(me, 2)
    partner = me + 1 - 2 * core
    x_dev = me + 2 - 4 * lax.rem(me // 2, 2)
    y_dev = me + 4 - 8 * (me // 4)

    def push(k, src, dst, dev):
        return pltpu.make_async_remote_copy(src_ref=src, dst_ref=dst, send_sem=sp_s.at[k], recv_sem=sp_r.at[k],
                                            device_id={"sp": dev}, device_id_type=MESH_ID)

    if part == 0:
        own = pltpu.make_async_copy(src_ref, all_ref.at[me], st_l.at[NB])
        spread = [push(k, src_ref, all_ref.at[me], dev) for k, dev in enumerate((x_dev, y_dev, partner))]
    else:
        lo, hi = pl.ds(0, FB // 2), pl.ds(FB // 2, FB // 2)
        far = x_dev + y_dev - me
        spread = [push(k, all_ref.at[at], all_ref.at[at], dev) for k, (at, dev) in enumerate(
            (((x_dev, lo), y_dev), ((y_dev, hi), x_dev), (x_dev, partner), (y_dev, partner)))]
        late = push(4, all_ref.at[far], all_ref.at[far], partner)

    def copies(b):
        row = core * NB + b
        return (pltpu.make_async_copy(buf_ref.at[b], st_ref.at[row], st_l.at[b]),
                pltpu.make_async_remote_copy(src_ref=buf_ref.at[b], dst_ref=st_ref.at[row], send_sem=st_s.at[b],
                                             recv_sem=st_r.at[b], device_id={"sp": partner}, device_id_type=MESH_ID))

    blocks = [load_block(0, (core * 2 + part) * NB + b, wu_ref, wd_ref, wu_buf.at[b], wd_buf.at[b], sem.at[b])
              for b in range(NB)]

    @pl.when(s == 0)
    def _():
        for block in blocks:
            for c in block:
                c.start()
        barrier = pltpu.get_barrier_semaphore()
        for dev in (x_dev, y_dev, partner):
            pl.semaphore_signal(barrier, inc=1, device_id={"sp": dev}, device_id_type=MESH_ID)
        pl.semaphore_wait(barrier, 3)
        if part == 0:
            own.start()
        for c in spread:
            c.start()

    if part == 1:
        @pl.when(s == 12)
        def _():
            spread[0].wait_recv()
            spread[1].wait_recv()
            late.start()

    for b in range(NB):
        @pl.when(s == b * NDEV)
        def _():
            dw_start(blocks[b], wu_buf.at[b], wut_ref, au_ref, ad_ref)

    @pl.when(s < NB * NDEV)
    def _():
        dw_tile(wut_ref[...], wd_buf[s // NDEV], n_ref[...].reshape(SEQ, D), g_ref[...].reshape(SEQ, D), au_ref, ad_ref)

    for b in range(NB):
        @pl.when(s == (b + 1) * NDEV - 1)
        def _():
            nu, nd = dw_finish(lr_ref[0], wut_ref[...], wd_buf[b], au_ref[...], ad_ref[...])
            buf_ref[b, 0:D] = nu
            buf_ref[b, D:D + FB] = nd[:, :FB]
            buf_ref[b, D + FB:] = nd[:, FB:]

        @pl.when(s == (b + 1) * NDEV)
        def _():
            for c in copies(b):
                c.start()

    @pl.when(s == NB * NDEV)
    def _():
        for b in range(NB):
            for c in copies(b):
                c.wait()
        if part == 0:
            for c in [own] + spread:
                c.wait()
        else:
            spread[0].wait_send()
            spread[1].wait_send()
            for c in spread[2:] + [late]:
                c.wait()


def dw_chip(part, lr, n_all, g4, wu, wd, spread):
    last = NB * NDEV - 1
    tile = lambda i: lax.rem(jnp.minimum(i, last), NDEV)
    return pl.pallas_call(
        functools.partial(dw_chip_kernel, part), grid=(NB * NDEV + 1,),
        in_specs=[SMEM, token_spec(n_all, tile), token_spec(g4, tile), ANY, ANY, ANY],
        out_specs=[ANY, ANY],
        out_shape=[jax.ShapeDtypeStruct((2 * NB, 2 * D, FB), BF), jax.ShapeDtypeStruct((NDEV, FB, D), BF)],
        input_output_aliases={5: 1} if part else {},
        scratch_shapes=[pltpu.VMEM((FB, D), BF), pltpu.VMEM((FB, D), F32), pltpu.VMEM((FB, D), F32),
                        pltpu.VMEM((NB, 2 * D, FB), BF), pltpu.VMEM((NB, D, FB), BF), pltpu.VMEM((NB, FB, D), BF)]
        + [pltpu.SemaphoreType.DMA((NB + 1,))] * 3 + [pltpu.SemaphoreType.DMA((NB, 2))] + [pltpu.SemaphoreType.DMA((NDEV,))] * 2,
        compiler_params=pltpu.CompilerParams(collective_id=12 + part, has_side_effects=True),
        cost_estimate=cost(NB * 8 * NDEV * SEQ * D * FB, 48),
        name="dw_chip",
    )(lr, n_all, g4, wu, wd, spread)


def dw_attn_kernel(l, lr_ref, n_ref, g_ref, d_ref, o_ref, wq_ref, wk_ref, wv_ref, wo_ref, w_ref, aq_ref, ao_ref, w_buf, wo_buf, sem):
    i = pl.program_id(0)
    at = pl.ds(pl.multiple_of(lax.axis_index("sp") * LANE, LANE), LANE)
    loads = [pltpu.make_async_copy(w.at[l, :, at], w_buf.at[k], sem.at[k]) for k, w in enumerate((wq_ref, wk_ref, wv_ref))]
    loads.append(pltpu.make_async_copy(wo_ref.at[l, at, :], wo_buf, sem.at[3]))

    @pl.when(i == 0)
    def _():
        for c in loads:
            c.start()
        aq_ref[...] = jnp.zeros_like(aq_ref)
        ao_ref[...] = jnp.zeros_like(ao_ref)

    aq_ref[...] += dot_nn(d_ref[...].T, n_ref[...].reshape(SEQ, D))
    ao_ref[...] += dot_nn(o_ref[...].T, g_ref[...].reshape(SEQ, D))

    @pl.when(i == pl.num_programs(0) - 1)
    def _():
        for c in loads:
            c.wait()
        lr = lr_ref[0]
        for k in range(3):
            at = slice(k * LANE, (k + 1) * LANE)
            w_ref[:, at] = (w_buf[k].astype(F32) - lr * aq_ref[at].T).astype(BF)
        no = (wo_buf[...].astype(F32) - lr * ao_ref[...]).astype(BF)
        for c in range(D // LANE):
            at = slice(c * LANE, (c + 1) * LANE)
            w_ref[at, QKV:512] = no[:, at]


def dw_attn(l, lr, n_all, g4, d_all, o_all, *weights):
    return pl.pallas_call(
        functools.partial(dw_attn_kernel, l), grid=(NDEV,),
        in_specs=[SMEM, token_spec(n_all), token_spec(g4), pl.BlockSpec((None, SEQ, QKV), lambda i: (i, 0, 0)),
                  pl.BlockSpec((None, SEQ, LANE), lambda i: (i, 0, 0))] + [ANY] * 4,
        out_specs=full(D, 512), out_shape=jax.ShapeDtypeStruct((D, 512), BF),
        scratch_shapes=[pltpu.VMEM((QKV, D), F32), pltpu.VMEM((LANE, D), F32), pltpu.VMEM((3, D, LANE), BF),
                        pltpu.VMEM((LANE, D), BF), pltpu.SemaphoreType.DMA((4,))],
        cost_estimate=cost(2 * NDEV * SEQ * D * 512, 24),
        name="dw_attn",
    )(lr, n_all, g4, d_all, o_all, *weights)


def norm_kernel(x_ref, gain_ref, n_ref):
    n_ref[...] = norm_apply(x_ref[...].astype(F32), gain_ref[...]).astype(BF)


def norm_tokens(x, gain_row):
    return pl.pallas_call(
        norm_kernel, grid=(NDEV,), in_specs=[pl.BlockSpec((SEQ, D), lambda i: (i, 0)), full(1, D)],
        out_specs=pl.BlockSpec((SEQ, D), lambda i: (i, 0)), out_shape=jax.ShapeDtypeStruct(x.shape, BF),
        cost_estimate=cost(1 << 28, 16), name="norm_tokens",
    )(x, gain_row)


def place_mlp_kernel(w_ref, *rest):
    u_ref, d_ref = rest[-2:]
    u_ref[...] = w_ref[0:D]
    d_ref[:, :FB] = w_ref[D:D + FB]
    d_ref[:, FB:] = w_ref[D + FB:]


def place_mlp(l, layers, w_all, prev, column):
    prev = list(prev)
    ff = NDEV * FB
    return pl.pallas_call(
        place_mlp_kernel, grid=(w_all.shape[0] // (2 * D),),
        in_specs=[pl.BlockSpec((2 * D, FB), lambda i: (i, 0))] + [ANY] * len(prev),
        out_specs=[pl.BlockSpec((None, D, FB), lambda i: (l, 0, column(i))), pl.BlockSpec((None, FB, D), lambda i: (l, column(i), 0))],
        out_shape=[jax.ShapeDtypeStruct((layers, D, ff), BF), jax.ShapeDtypeStruct((layers, ff, D), BF)],
        input_output_aliases={1 + i: i for i in range(len(prev))},
        cost_estimate=cost(1 << 30, 32),
        name="place_mlp",
    )(w_all, *prev)


def place_kernel(w_ref, prev_ref, o_ref):
    o_ref[...] = w_ref[...]


def place_up(l, w_all, prev):
    return pl.pallas_call(
        place_kernel, grid=(NDEV,), in_specs=[pl.BlockSpec((D, FB), lambda i: (i, 0)), ANY],
        out_specs=pl.BlockSpec((None, D, FB), lambda i: (l, 0, i)), out_shape=jax.ShapeDtypeStruct(prev.shape, BF),
        input_output_aliases={1: 0}, cost_estimate=cost(1 << 29, 16), name="place_up",
    )(w_all, prev)


def place_down(l, w_all, prev):
    return pl.pallas_call(
        place_kernel, grid=(NDEV,), in_specs=[pl.BlockSpec((FB, D), lambda i: (i, 0)), ANY],
        out_specs=pl.BlockSpec((None, FB, D), lambda i: (l, i, 0)), out_shape=jax.ShapeDtypeStruct(prev.shape, BF),
        input_output_aliases={1: 0}, cost_estimate=cost(1 << 29, 16), name="place_down",
    )(w_all, prev)


def place_attn_kernel(w_ref, *rest):
    q_ref, k_ref, v_ref, o_ref = rest[-4:]
    q_ref[...] = w_ref[:, 0:LANE]
    k_ref[...] = w_ref[:, LANE:256]
    v_ref[...] = w_ref[:, 256:QKV]
    for c in range(D // LANE):
        o_ref[:, c * LANE:(c + 1) * LANE] = w_ref[c * LANE:(c + 1) * LANE, QKV:512]


def place_attn(l, layers, w_all, prev):
    prev = list(prev)
    col = pl.BlockSpec((None, D, LANE), lambda i: (l, 0, i))
    return pl.pallas_call(
        place_attn_kernel, grid=(NDEV,),
        in_specs=[pl.BlockSpec((D, 512), lambda i: (i, 0))] + [ANY] * len(prev),
        out_specs=[col, col, col, pl.BlockSpec((None, LANE, D), lambda i: (l, i, 0))],
        out_shape=[jax.ShapeDtypeStruct((layers, D, D), BF)] * 4,
        input_output_aliases={1 + i: i for i in range(len(prev))},
        cost_estimate=cost(1 << 30, 16),
        name="place_attn",
    )(w_all, *prev)


def solution(mesh):
    act_spec = P("dp", "sp", None)
    out_four = P("dp", None, None, None)
    out_three = P("dp", None, None)

    def step(hidden_in, positions, grad_y, w_query, w_key, w_value, w_out, w_up, w_down, gain, learn_rate):
        layers = w_query.shape[0]
        idx = lax.axis_index("sp")
        chunk = SEQ // NDEV
        lr = learn_rate.reshape(1)

        def gather(t):
            return lax.all_gather(t, "sp", axis=0, tiled=True)

        def swap(t):
            return lax.all_to_all(t, "sp", 0, 0, tiled=True)

        def own(t):
            return lax.dynamic_index_in_dim(t, idx, 1, keepdims=False).reshape(SEQ, D)

        pos_tile = jnp.zeros((8, LANE), jnp.int32).at[0, :chunk].set(positions)
        pos = share(jnp.broadcast_to(pos_tile, (NDEV, 8, LANE)))[:, 0, :chunk].reshape(SEQ)

        x_all = lax.all_gather(hidden_in, "sp", axis=0, tiled=False)
        gy_all = lax.all_gather(grad_y, "sp", axis=0, tiled=False)
        lane = jnp.arange(LANE, dtype=jnp.int32)
        freqs = ROPE_BASE ** (-(lane % (HD // 2)).astype(F32) / (HD // 2))
        angles = pos.astype(F32)[:, None] * freqs[None, :]
        c_tab = jnp.cos(angles)
        s_tab = jnp.sin(angles) * jnp.where(lane % HD < HD // 2, -1.0, 1.0)[None, :]

        wq = w_query.reshape(layers, D, D)
        wk = w_key.reshape(layers, D, D)
        wv = w_value.reshape(layers, D, D)
        wo = w_out.reshape(layers, D, D)

        def gain_row(l):
            return gain[l].reshape(1, D)

        x0 = own(x_all)
        n0 = norm_apply(x0.astype(F32), gain[0]).astype(BF)
        q0, k0, v0, o0, o_pack0, lse0 = attn_fwd(0, n0, wq, wk, wv, c_tab, s_tab)
        o_all0 = swap(o_pack0)
        pre0, x1, n1 = mlp_fwd(0, False, n0, x0, o0, wo, w_up, w_down, gain_row(1))
        n1_all = gather(n1).reshape(1, NDEV, SEQ, D)
        q1, k1, v1, o1, o_pack1, lse1 = attn_fwd(1, n1, wq, wk, wv, c_tab, s_tab)
        o_all1 = swap(o_pack1)
        pre1, y = mlp_fwd(1, True, n1, x1, o1, wo, w_up, w_down, gain_row(1))
        out_y = swap(y.reshape(NDEV, chunk, D))

        gy = own(gy_all)
        dn1, d_pack1 = attn_bwd(1, gy, wo, wq, wk, wv, q1, k1, v1, lse1, c_tab, s_tab)
        d_all1 = swap(d_pack1)
        g0 = mlp_bwd(1, gy, pre1, w_up, w_down, dn1, x1, gain_row(1))
        g0_all = gather(g0).reshape(1, NDEV, SEQ, D)
        tie = lax.optimization_barrier

        dn0, d_pack0 = attn_bwd(0, g0, wo, wq, wk, wv, q0, k0, v0, lse0, c_tab, s_tab)
        d_all0 = swap(d_pack0)
        d_all1, dn0 = tie((d_all1, dn0))
        w_attn1 = dw_attn(1, lr, n1_all, gy_all, d_all1, o_all1, wq, wk, wv, wo)
        w_attn1_all = gather(w_attn1)
        dn0, w_attn1 = tie((dn0, w_attn1))
        gx = mlp_bwd(0, g0, pre0, w_up, w_down, dn0, x0, gain_row(0))
        grad_x = swap(gx.reshape(NDEV, chunk, D))
        gy_all, gx = tie((gy_all, gx))
        w_up1, w_mlp1 = dw_mlp(1, lr, n1_all, gy_all, w_up, w_down)
        w_up1_all = gather(w_up1)
        x_all, w_mlp1 = tie((x_all, w_mlp1))
        n0_all = norm_tokens(x_all.reshape(NDEV * SEQ, D), gain_row(0)).reshape(x_all.shape)
        w_attn0 = dw_attn(0, lr, n0_all, g0_all, d_all0, o_all0, wq, wk, wv, wo)
        w_attn0_all = gather(w_attn0)
        n0_all, w_attn0 = tie((n0_all, w_attn0))
        st0, w_down1 = dw_chip(0, lr, n0_all, g0_all, w_up, w_down, w_mlp1)
        n0_all, st0 = tie((n0_all, st0))
        st1, w_down1 = dw_chip(1, lr, n0_all, g0_all, w_up, w_down, w_down1)
        up_down = ()
        for a, st in enumerate((st0, st1)):
            up_down = place_mlp(0, layers, st.reshape(2 * NB * 2 * D, FB), up_down,
                                lambda i, a=a: (i // NB) * 2 * NB + a * NB + lax.rem(i, NB))
        attn_new = place_attn(1, layers, w_attn1_all, ())
        attn_new = place_attn(0, layers, w_attn0_all, attn_new)
        new_down = place_down(1, w_down1.reshape(NDEV * FB, D), up_down[1])
        new_up = place_up(1, w_up1_all, up_down[0])
        nq, nk, nv, no = attn_new
        return (out_y, grad_x, nq.reshape(w_query.shape), nk.reshape(w_query.shape), nv.reshape(w_query.shape),
                no.reshape(w_out.shape), new_up, new_down)

    return jax.shard_map(step, mesh=mesh,
                         in_specs=(act_spec, P(("dp", "sp")), act_spec, P(), P(), P(), P(), P(), P(), P(), P()),
                         out_specs=(act_spec, act_spec, out_four, out_four, out_four, out_four, out_three, out_three),
                         check_vma=False)
```

```python
import functools
import jax
import jax.numpy as jnp
from jax import lax
from jax.experimental import pallas as pl
from jax.experimental.pallas import tpu as pltpu
from jax.sharding import PartitionSpec as P

EPSILON = 1e-6
ROPE_BASE = 10000.0
NEG_LARGE = -1e30
HD = 64
SEQ = 512
LANE = 128
QKV = 384
D = 1024
CB = 256
QB = 256
BF = jnp.bfloat16
F32 = jnp.float32


ANY = pl.BlockSpec(memory_space=pl.ANY)
SMEM = pl.BlockSpec(memory_space=pltpu.SMEM)


def full(*shape):
    return pl.BlockSpec(shape, lambda i: (0, 0))


def cost(flops, mib):
    return pl.CostEstimate(flops=flops, bytes_accessed=mib << 20, transcendentals=0)


def norm_apply(x_f32, gain_row):
    inv_rms = lax.rsqrt(jnp.mean(x_f32 * x_f32, axis=-1, keepdims=True) + EPSILON)
    return x_f32 * inv_rms * gain_row


def dot_nn(a, b):
    return lax.dot_general(a, b, (((1,), (0,)), ((), ())), preferred_element_type=F32)


def dot_nt(a, b):
    return lax.dot_general(a, b, (((1,), (1,)), ((), ())), preferred_element_type=F32)


def swap_halves(t):
    lane = lax.broadcasted_iota(jnp.int32, t.shape, 1)
    return jnp.where(lane % HD < HD // 2, pltpu.roll(t, t.shape[1] - HD // 2, 1), pltpu.roll(t, HD // 2, 1))


def head_mask(rows, h):
    lane = lax.broadcasted_iota(jnp.int32, (rows, LANE), 1)
    return lane < HD if h % 2 == 0 else lane >= HD


def causal_mask(nk, j):
    key = lax.broadcasted_iota(jnp.int32, (nk, QB), 0)
    qry = lax.broadcasted_iota(jnp.int32, (nk, QB), 1) + j * QB
    return key <= qry


def attn_fwd_kernel(n_ref, wq_ref, wk_ref, wv_ref, c_ref, s_ref, q_ref, k_ref, v_ref, o_ref, op_ref, lse_ref):
    n = n_ref[...]
    c = jnp.concatenate([c_ref[...]] * (CB // LANE), axis=1)
    s = jnp.concatenate([s_ref[...]] * (CB // LANE), axis=1)
    qf = dot_nn(n, wq_ref[...])
    q = (qf * c + swap_halves(qf) * s).astype(BF)
    kf = dot_nn(n, wk_ref[...])
    k = (kf * c + swap_halves(kf) * s).astype(BF)
    v = dot_nn(n, wv_ref[...]).astype(BF)
    q_ref[...] = q
    k_ref[...] = k
    v_ref[...] = v
    vt = v.T
    heads = []
    for h in range(CB // HD):
        lo = (h // 2) * LANE
        qm = jnp.where(head_mask(SEQ, h), q[:, lo:lo + LANE] * BF(HD ** -0.5), BF(0))
        k2 = k[:, lo:lo + LANE]
        cols = []
        for j in range(SEQ // QB):
            nk = (j + 1) * QB
            st = dot_nt(k2[:nk], qm[j * QB:(j + 1) * QB])
            st = jnp.where(causal_mask(nk, j), st, NEG_LARGE)
            m = jnp.max(st, axis=0, keepdims=True)
            e = jnp.exp(st - m)
            l = jnp.sum(e, axis=0, keepdims=True)
            p = (e * (1.0 / l)).astype(BF)
            cols.append(dot_nn(vt[h * HD:(h + 1) * HD, :nk], p))
            lse_ref[h:h + 1, j * QB:(j + 1) * QB] = m + jnp.log(l)
        heads.append(jnp.concatenate(cols, axis=1))
    o = jnp.concatenate(heads, axis=0).T.astype(BF)
    o_ref[...] = o
    op_ref[0] = o[:, :LANE]
    op_ref[1] = o[:, LANE:]


def attn_fwd(l, n, wq, wk, wv, c, s):
    nb = D // CB
    wspec = pl.BlockSpec((None, D, CB), lambda i: (l, 0, i))
    aspec = pl.BlockSpec((SEQ, CB), lambda i: (0, i))
    act = jax.ShapeDtypeStruct((SEQ, D), BF)
    return pl.pallas_call(
        attn_fwd_kernel,
        grid=(nb,),
        in_specs=[full(SEQ, D), wspec, wspec, wspec, full(SEQ, LANE), full(SEQ, LANE)],
        out_specs=[aspec, aspec, aspec, aspec, pl.BlockSpec((2, SEQ, LANE), lambda i: (i, 0, 0)),
                   pl.BlockSpec((None, CB // HD, SEQ), lambda i: (i, 0, 0))],
        out_shape=[act, act, act, act, jax.ShapeDtypeStruct((8, SEQ, LANE), BF),
                   jax.ShapeDtypeStruct((nb, CB // HD, SEQ), F32)],
        cost_estimate=cost(6 * SEQ * D * D + 8 * SEQ * SEQ * D, 14),
        name="attn_fwd",
    )(n, wq, wk, wv, c, s)


def attn_bwd_kernel(g_ref, wo_ref, wq_ref, wk_ref, wv_ref, q_ref, k_ref, v_ref, lse_ref, c_ref, s_ref, dn_ref, dp_ref):
    do = dot_nt(g_ref[...], wo_ref[...]).astype(BF)
    q = q_ref[...]
    k = k_ref[...]
    v = v_ref[...]
    kt = k.T
    dqs, dks, dvs = [], [], []
    for h in range(CB // HD):
        lo = (h // 2) * LANE
        hm = head_mask(SEQ, h)
        q2 = q[:, lo:lo + LANE]
        qm = jnp.where(hm, q2 * BF(HD ** -0.5), BF(0))
        do2 = do[:, lo:lo + LANE]
        dom = jnp.where(hm, do2, BF(0))
        k2 = k[:, lo:lo + LANE]
        v2 = v[:, lo:lo + LANE]
        dk = dv = None
        cols = []
        for j in reversed(range(SEQ // QB)):
            nk = (j + 1) * QB
            rows = slice(j * QB, (j + 1) * QB)
            st = dot_nt(k2[:nk], qm[rows])
            pt = jnp.where(causal_mask(nk, j), jnp.exp(st - lse_ref[h:h + 1, rows]), 0.0)
            dpt = dot_nt(v2[:nk], dom[rows])
            rd = jnp.sum(dpt * pt, axis=0, keepdims=True)
            dst = (pt * (dpt - rd) * HD ** -0.5).astype(BF)
            dv_j = dot_nn(pt.astype(BF), do2[rows])
            dk_j = dot_nn(dst, q2[rows])
            cols.append(dot_nn(kt[h * HD:(h + 1) * HD, :nk], dst))
            if dk is None:
                dk, dv = dk_j, dv_j
            else:
                dk = jnp.concatenate([dk[:nk] + dk_j, dk[nk:]], axis=0)
                dv = jnp.concatenate([dv[:nk] + dv_j, dv[nk:]], axis=0)
        dqs.append(jnp.concatenate(cols[::-1], axis=1))
        dks.append(dk)
        dvs.append(dv)
    c = jnp.concatenate([c_ref[...]] * (CB // LANE), axis=1)
    s = jnp.concatenate([s_ref[...]] * (CB // LANE), axis=1)
    low = head_mask(SEQ, 0)

    def join(parts):
        return jnp.concatenate([jnp.where(low, parts[2 * i], parts[2 * i + 1]) for i in range(CB // LANE)], axis=1).astype(BF)

    def unrope(t):
        t = t.astype(F32)
        return (t * c - swap_halves(t) * s).astype(BF)

    dq = unrope(jnp.concatenate(dqs, axis=0).T.astype(BF))
    dk = unrope(join(dks))
    dv = join(dvs)
    for i in range(2):
        dp_ref[i, :, 0:LANE] = dq[:, i * LANE:(i + 1) * LANE]
        dp_ref[i, :, LANE:256] = dk[:, i * LANE:(i + 1) * LANE]
        dp_ref[i, :, 256:QKV] = dv[:, i * LANE:(i + 1) * LANE]
    dn = dot_nt(dq, wq_ref[...]) + dot_nt(dk, wk_ref[...]) + dot_nt(dv, wv_ref[...])

    @pl.when(pl.program_id(0) == 0)
    def _():
        dn_ref[...] = dn

    @pl.when(pl.program_id(0) > 0)
    def _():
        dn_ref[...] += dn


def attn_bwd(l, g, wo, wq, wk, wv, q, k, v, lse, c, s):
    nb = D // CB
    wspec = pl.BlockSpec((None, D, CB), lambda i: (l, 0, i))
    aspec = pl.BlockSpec((SEQ, CB), lambda i: (0, i))
    return pl.pallas_call(
        attn_bwd_kernel,
        grid=(nb,),
        in_specs=[full(SEQ, D), pl.BlockSpec((None, CB, D), lambda i: (l, i, 0)), wspec, wspec, wspec, aspec, aspec, aspec,
                  pl.BlockSpec((None, CB // HD, SEQ), lambda i: (i, 0, 0)), full(SEQ, LANE), full(SEQ, LANE)],
        out_specs=[full(SEQ, D), pl.BlockSpec((2, SEQ, QKV), lambda i: (i, 0, 0))],
        out_shape=[jax.ShapeDtypeStruct((SEQ, D), F32), jax.ShapeDtypeStruct((8, SEQ, QKV), BF)],
        cost_estimate=cost(8 * SEQ * D * D + 20 * SEQ * SEQ * D, 20),
        name="attn_bwd",
    )(g, wo, wq, wk, wv, q, k, v, lse, c, s)


NDEV = 8
MB = 1024
MESH_ID = pl.DeviceIdType.MESH
FB = 512


def token_spec(t, tile=lambda i: i):
    return pl.BlockSpec((t.shape[0], None, t.shape[2], D), lambda i: (0, tile(i), 0, 0))


class Exchange:
    def __init__(self, pairs, send_sem, recv_sem, local_sem):
        me = lax.axis_index("sp")
        self.remote, self.local = [], []
        for a, (src, dst) in enumerate(pairs):
            self.local.append(pltpu.make_async_copy(src.at[me], dst.at[me], local_sem.at[a]))
        for k in range(1, NDEV):
            peer = lax.rem(me + k, NDEV)
            for a, (src, dst) in enumerate(pairs):
                self.remote.append(pltpu.make_async_remote_copy(
                    src_ref=src.at[peer], dst_ref=dst.at[me], send_sem=send_sem.at[a, k], recv_sem=recv_sem.at[a, k],
                    device_id={"sp": peer}, device_id_type=MESH_ID))

    def start(self):
        me = lax.axis_index("sp")
        barrier = pltpu.get_barrier_semaphore()
        for k in range(1, NDEV):
            pl.semaphore_signal(barrier, inc=1, device_id={"sp": lax.rem(me + k, NDEV)}, device_id_type=MESH_ID)
        for c in self.local:
            c.start()
        pl.semaphore_wait(barrier, NDEV - 1)
        for c in self.remote:
            c.start()

    def wait(self):
        for c in self.local + self.remote:
            c.wait()


def exchange_sems(n):
    return [pltpu.SemaphoreType.DMA((n, NDEV)), pltpu.SemaphoreType.DMA((n, NDEV)), pltpu.SemaphoreType.DMA((n,))]


def share_kernel(p_ref, po_ref, ss, rs, ls):
    ex = Exchange([(p_ref, po_ref)], ss, rs, ls)
    ex.start()
    ex.wait()


def share(pos):
    return pl.pallas_call(
        share_kernel, in_specs=[ANY], out_specs=ANY, out_shape=jax.ShapeDtypeStruct(pos.shape, pos.dtype),
        scratch_shapes=exchange_sems(1),
        compiler_params=pltpu.CompilerParams(collective_id=1, has_side_effects=True), name="share",
    )(pos)


def gelu_parts(x):
    c = 0.7978845608028654
    x2 = x * x
    t = jnp.tanh(c * (x + 0.044715 * (x2 * x)))
    return x2, t, c


def gelu(x):
    _, t, _ = gelu_parts(x)
    return x * (0.5 * (1.0 + t))


def gelu_slope(x):
    x2, t, c = gelu_parts(x)
    return 0.5 * (1.0 + t) + 0.5 * x * (1.0 - t * t) * (c * (1.0 + 3 * 0.044715 * x2))


def mlp_fwd_kernel(last, n_ref, x_ref, o_ref, wo_ref, wu_ref, wd_ref, gain_ref, *rest):
    if last:
        pre_ref, h_ref, acc_ref = rest
    else:
        pre_ref, h_ref, nn_ref, acc_ref = rest
    i = pl.program_id(0)

    @pl.when(i == 0)
    def _():
        acc_ref[...] = x_ref[...].astype(F32) + dot_nn(o_ref[...], wo_ref[...])

    pre = dot_nn(n_ref[...], wu_ref[...])
    pre_ref[...] = pre
    acc_ref[...] += dot_nn(gelu(pre).astype(BF), wd_ref[...])

    @pl.when(i == pl.num_programs(0) - 1)
    def _():
        h = acc_ref[...].astype(BF)
        h_ref[...] = h
        if not last:
            nn_ref[...] = norm_apply(h.astype(F32), gain_ref[...]).astype(BF)


def mlp_fwd(l, last, n, x, o, wo, wu, wd, gain_next):
    ff = wu.shape[2]
    act = jax.ShapeDtypeStruct((SEQ, D), BF)
    out_specs = [pl.BlockSpec((SEQ, MB), lambda i: (0, i)), full(SEQ, D)]
    out_shape = [jax.ShapeDtypeStruct((SEQ, ff), F32), act]
    if not last:
        out_specs.append(full(SEQ, D))
        out_shape.append(act)
    return pl.pallas_call(
        functools.partial(mlp_fwd_kernel, last), grid=(ff // MB,),
        in_specs=[full(SEQ, D), full(SEQ, D), full(SEQ, D), pl.BlockSpec((None, D, D), lambda i: (l, 0, 0)),
                  pl.BlockSpec((None, D, MB), lambda i: (l, 0, i)), pl.BlockSpec((None, MB, D), lambda i: (l, i, 0)),
                  full(1, D)],
        out_specs=out_specs, out_shape=out_shape,
        scratch_shapes=[pltpu.VMEM((SEQ, D), F32)],
        cost_estimate=cost(4 * SEQ * D * ff + 2 * SEQ * D * D, 30),
        name="mlp_fwd",
    )(n, x, o, wo, wu, wd, gain_next)


def mlp_bwd_kernel(g_ref, pre_ref, wu_ref, wd_ref, dn_ref, x_ref, gain_ref, go_ref, acc_ref):
    i = pl.program_id(0)

    @pl.when(i == 0)
    def _():
        acc_ref[...] = dn_ref[...]

    d_act = dot_nt(g_ref[...], wd_ref[...]).astype(BF)
    d_pre = (d_act.astype(F32) * gelu_slope(pre_ref[...])).astype(BF)
    acc_ref[...] += dot_nt(d_pre, wu_ref[...])

    @pl.when(i == pl.num_programs(0) - 1)
    def _():
        x = x_ref[...].astype(F32)
        r = lax.rsqrt(jnp.mean(x * x, axis=-1, keepdims=True) + EPSILON)
        t = acc_ref[...] * gain_ref[...]
        dot = jnp.mean(x * t, axis=-1, keepdims=True)
        dx = r * t - x * (r * r * r * dot)
        go_ref[...] = (g_ref[...].astype(F32) + dx).astype(BF)


def mlp_bwd(l, g, pre, wu, wd, dn, x, gain_row):
    ff = wu.shape[2]
    return pl.pallas_call(
        mlp_bwd_kernel, grid=(ff // MB,),
        in_specs=[full(SEQ, D), pl.BlockSpec((SEQ, MB), lambda i: (0, i)), pl.BlockSpec((None, D, MB), lambda i: (l, 0, i)),
                  pl.BlockSpec((None, MB, D), lambda i: (l, i, 0)), full(SEQ, D), full(SEQ, D), full(1, D)],
        out_specs=full(SEQ, D), out_shape=jax.ShapeDtypeStruct((SEQ, D), BF),
        scratch_shapes=[pltpu.VMEM((SEQ, D), F32)],
        cost_estimate=cost(4 * SEQ * D * ff, 30),
        name="mlp_bwd",
    )(g, pre, wu, wd, dn, x, gain_row)


def dw_tile(wut, wd, n, g, au_ref, ad_ref):
    pre = dot_nt(wut, n)
    d_act = dot_nt(wd, g).astype(BF)
    x2, t, c = gelu_parts(pre)
    half = 0.5 * (1.0 + t)
    act = (pre * half).astype(BF)
    slope = half + 0.5 * pre * (1.0 - t * t) * (c * (1.0 + 3 * 0.044715 * x2))
    d_pre = (d_act.astype(F32) * slope).astype(BF)
    ad_ref[...] += dot_nn(act, g)
    au_ref[...] += dot_nn(d_pre, n)


def dw_finish(lr, wut, wd, au, ad):
    nu = (wut.astype(F32) - lr * au).astype(BF).T
    nd = (wd.astype(F32) - lr * ad).astype(BF)
    return nu, nd


def load_block(l, col, wu_ref, wd_ref, wu_buf, wd_buf, sem):
    at = pl.ds(pl.multiple_of(col * FB, FB), FB)
    return (pltpu.make_async_copy(wu_ref.at[l, :, at], wu_buf, sem.at[0]),
            pltpu.make_async_copy(wd_ref.at[l, at, :], wd_buf, sem.at[1]))


def dw_start(block, wu, wut_ref, au_ref, ad_ref):
    for c in block:
        c.wait()
    wut_ref[...] = wu[...].T
    au_ref[...] = jnp.zeros_like(au_ref)
    ad_ref[...] = jnp.zeros_like(ad_ref)


def dw_mlp_kernel(l, lr_ref, n_ref, g_ref, wu_ref, wd_ref, nu_ref, nd_ref, wut_ref, au_ref, ad_ref, wu_buf, wd_buf, sem):
    i = pl.program_id(0)

    @pl.when(i == 0)
    def _():
        block = load_block(l, lax.axis_index("sp"), wu_ref, wd_ref, wu_buf, wd_buf, sem)
        for c in block:
            c.start()
        dw_start(block, wu_buf, wut_ref, au_ref, ad_ref)

    dw_tile(wut_ref[...], wd_buf[...], n_ref[...].reshape(SEQ, D), g_ref[...].reshape(SEQ, D), au_ref, ad_ref)

    @pl.when(i == pl.num_programs(0) - 1)
    def _():
        nu_ref[...], nd_ref[...] = dw_finish(lr_ref[0], wut_ref[...], wd_buf[...], au_ref[...], ad_ref[...])


def dw_mlp(l, lr, n_all, g4, wu, wd):
    return pl.pallas_call(
        functools.partial(dw_mlp_kernel, l), grid=(NDEV,),
        in_specs=[SMEM, token_spec(n_all), token_spec(g4), ANY, ANY],
        out_specs=[full(D, FB), full(FB, D)], out_shape=[jax.ShapeDtypeStruct((D, FB), BF), jax.ShapeDtypeStruct((FB, D), BF)],
        scratch_shapes=[pltpu.VMEM((FB, D), BF), pltpu.VMEM((FB, D), F32), pltpu.VMEM((FB, D), F32),
                        pltpu.VMEM((D, FB), BF), pltpu.VMEM((FB, D), BF), pltpu.SemaphoreType.DMA((2,))],
        cost_estimate=cost(8 * NDEV * SEQ * D * FB, 24),
        name="dw_mlp",
    )(lr, n_all, g4, wu, wd)


NB = 4


def dw_chip_kernel(lr_ref, n_ref, g_ref, wu_ref, wd_ref, src_ref, st_ref, all_ref, wut_ref, au_ref, ad_ref, buf_ref,
                   wu_buf, wd_buf, st_s, st_r, st_l, sem, sp_s, sp_r):
    s = pl.program_id(0)
    me = lax.axis_index("sp")
    core = lax.rem(me, 2)
    partner = me + 1 - 2 * core
    x_dev = me + 2 - 4 * lax.rem(me // 2, 2)
    y_dev = me + 4 - 8 * (me // 4)

    def push(k, src, dst, dev):
        return pltpu.make_async_remote_copy(src_ref=src, dst_ref=dst, send_sem=sp_s.at[k], recv_sem=sp_r.at[k],
                                            device_id={"sp": dev}, device_id_type=MESH_ID)

    lo, hi = pl.ds(0, FB // 2), pl.ds(FB // 2, FB // 2)
    far = x_dev + y_dev - me
    own = pltpu.make_async_copy(src_ref, all_ref.at[me], st_l.at[NB])
    first = [push(k, src_ref, all_ref.at[me], dev) for k, dev in enumerate((x_dev, y_dev, partner))]
    second = [push(3 + k, all_ref.at[at], all_ref.at[at], dev) for k, (at, dev) in enumerate(
        (((x_dev, lo), y_dev), ((y_dev, hi), x_dev), (x_dev, partner), (y_dev, partner)))]
    third = push(7, all_ref.at[far], all_ref.at[far], partner)

    def copies(b):
        row = core * NB + b
        return (pltpu.make_async_copy(buf_ref.at[b], st_ref.at[row], st_l.at[b]),
                pltpu.make_async_remote_copy(src_ref=buf_ref.at[b], dst_ref=st_ref.at[row], send_sem=st_s.at[b],
                                             recv_sem=st_r.at[b], device_id={"sp": partner}, device_id_type=MESH_ID))

    blocks = [load_block(0, core * NB + b, wu_ref, wd_ref, wu_buf.at[b], wd_buf.at[b], sem.at[b])
              for b in range(NB)]

    @pl.when(s == 0)
    def _():
        for block in blocks:
            for c in block:
                c.start()
        barrier = pltpu.get_barrier_semaphore()
        for dev in (x_dev, y_dev, partner):
            pl.semaphore_signal(barrier, inc=1, device_id={"sp": dev}, device_id_type=MESH_ID)
        pl.semaphore_wait(barrier, 3)
        own.start()
        for c in first:
            c.start()

    @pl.when(s == 18)
    def _():
        first[0].wait_recv()
        first[1].wait_recv()
        for c in second:
            c.start()

    @pl.when(s == 27)
    def _():
        second[0].wait_recv()
        second[1].wait_recv()
        third.start()

    for b in range(NB):
        @pl.when(s == b * NDEV)
        def _():
            dw_start(blocks[b], wu_buf.at[b], wut_ref, au_ref, ad_ref)

    @pl.when(s < NB * NDEV)
    def _():
        dw_tile(wut_ref[...], wd_buf[s // NDEV], n_ref[...].reshape(SEQ, D), g_ref[...].reshape(SEQ, D), au_ref, ad_ref)

    for b in range(NB):
        @pl.when(s == (b + 1) * NDEV - 1)
        def _():
            nu, nd = dw_finish(lr_ref[0], wut_ref[...], wd_buf[b], au_ref[...], ad_ref[...])
            buf_ref[b, 0:D] = nu
            buf_ref[b, D:D + FB] = nd[:, :FB]
            buf_ref[b, D + FB:] = nd[:, FB:]

        @pl.when(s == (b + 1) * NDEV)
        def _():
            for c in copies(b):
                c.start()

    @pl.when(s == NB * NDEV)
    def _():
        for b in range(NB):
            for c in copies(b):
                c.wait()
        for c in first[:2] + second[:2]:
            c.wait_send()
        for c in [own, first[2], third] + second[2:]:
            c.wait()


def dw_chip(lr, n_all, g4, wu, wd, spread):
    last = NB * NDEV - 1
    tile = lambda i: lax.rem(jnp.minimum(i, last), NDEV)
    return pl.pallas_call(
        dw_chip_kernel, grid=(NB * NDEV + 1,),
        in_specs=[SMEM, token_spec(n_all, tile), token_spec(g4, tile), ANY, ANY, ANY],
        out_specs=[ANY, ANY],
        out_shape=[jax.ShapeDtypeStruct((2 * NB, 2 * D, FB), BF), jax.ShapeDtypeStruct((NDEV, FB, D), BF)],
        scratch_shapes=[pltpu.VMEM((FB, D), BF), pltpu.VMEM((FB, D), F32), pltpu.VMEM((FB, D), F32),
                        pltpu.VMEM((NB, 2 * D, FB), BF), pltpu.VMEM((NB, D, FB), BF), pltpu.VMEM((NB, FB, D), BF)]
        + [pltpu.SemaphoreType.DMA((NB + 1,))] * 3 + [pltpu.SemaphoreType.DMA((NB, 2))] + [pltpu.SemaphoreType.DMA((NDEV,))] * 2,
        compiler_params=pltpu.CompilerParams(collective_id=12, has_side_effects=True),
        cost_estimate=cost(NB * 8 * NDEV * SEQ * D * FB, 48),
        name="dw_chip",
    )(lr, n_all, g4, wu, wd, spread)


def dw_attn_kernel(l, lr_ref, n_ref, g_ref, d_ref, o_ref, wq_ref, wk_ref, wv_ref, wo_ref, w_ref, aq_ref, ao_ref, w_buf, wo_buf, sem):
    i = pl.program_id(0)
    at = pl.ds(pl.multiple_of(lax.axis_index("sp") * LANE, LANE), LANE)
    loads = [pltpu.make_async_copy(w.at[l, :, at], w_buf.at[k], sem.at[k]) for k, w in enumerate((wq_ref, wk_ref, wv_ref))]
    loads.append(pltpu.make_async_copy(wo_ref.at[l, at, :], wo_buf, sem.at[3]))

    @pl.when(i == 0)
    def _():
        for c in loads:
            c.start()
        aq_ref[...] = jnp.zeros_like(aq_ref)
        ao_ref[...] = jnp.zeros_like(ao_ref)

    aq_ref[...] += dot_nn(d_ref[...].T, n_ref[...].reshape(SEQ, D))
    ao_ref[...] += dot_nn(o_ref[...].T, g_ref[...].reshape(SEQ, D))

    @pl.when(i == pl.num_programs(0) - 1)
    def _():
        for c in loads:
            c.wait()
        lr = lr_ref[0]
        for k in range(3):
            at = slice(k * LANE, (k + 1) * LANE)
            w_ref[:, at] = (w_buf[k].astype(F32) - lr * aq_ref[at].T).astype(BF)
        no = (wo_buf[...].astype(F32) - lr * ao_ref[...]).astype(BF)
        for c in range(D // LANE):
            at = slice(c * LANE, (c + 1) * LANE)
            w_ref[at, QKV:512] = no[:, at]


def dw_attn(l, lr, n_all, g4, d_all, o_all, *weights):
    return pl.pallas_call(
        functools.partial(dw_attn_kernel, l), grid=(NDEV,),
        in_specs=[SMEM, token_spec(n_all), token_spec(g4), pl.BlockSpec((None, SEQ, QKV), lambda i: (i, 0, 0)),
                  pl.BlockSpec((None, SEQ, LANE), lambda i: (i, 0, 0))] + [ANY] * 4,
        out_specs=full(D, 512), out_shape=jax.ShapeDtypeStruct((D, 512), BF),
        scratch_shapes=[pltpu.VMEM((QKV, D), F32), pltpu.VMEM((LANE, D), F32), pltpu.VMEM((3, D, LANE), BF),
                        pltpu.VMEM((LANE, D), BF), pltpu.SemaphoreType.DMA((4,))],
        cost_estimate=cost(2 * NDEV * SEQ * D * 512, 24),
        name="dw_attn",
    )(lr, n_all, g4, d_all, o_all, *weights)


def norm_kernel(x_ref, gain_ref, n_ref):
    n_ref[...] = norm_apply(x_ref[...].astype(F32), gain_ref[...]).astype(BF)


def norm_tokens(x, gain_row):
    return pl.pallas_call(
        norm_kernel, grid=(NDEV,), in_specs=[pl.BlockSpec((SEQ, D), lambda i: (i, 0)), full(1, D)],
        out_specs=pl.BlockSpec((SEQ, D), lambda i: (i, 0)), out_shape=jax.ShapeDtypeStruct(x.shape, BF),
        cost_estimate=cost(1 << 28, 16), name="norm_tokens",
    )(x, gain_row)


def place_mlp_kernel(w_ref, *rest):
    u_ref, d_ref = rest[-2:]
    u_ref[...] = w_ref[0:D]
    d_ref[:, :FB] = w_ref[D:D + FB]
    d_ref[:, FB:] = w_ref[D + FB:]


def place_mlp(l, layers, w_all, prev, column):
    prev = list(prev)
    ff = NDEV * FB
    return pl.pallas_call(
        place_mlp_kernel, grid=(w_all.shape[0] // (2 * D),),
        in_specs=[pl.BlockSpec((2 * D, FB), lambda i: (i, 0))] + [ANY] * len(prev),
        out_specs=[pl.BlockSpec((None, D, FB), lambda i: (l, 0, column(i))), pl.BlockSpec((None, FB, D), lambda i: (l, column(i), 0))],
        out_shape=[jax.ShapeDtypeStruct((layers, D, ff), BF), jax.ShapeDtypeStruct((layers, ff, D), BF)],
        input_output_aliases={1 + i: i for i in range(len(prev))},
        cost_estimate=cost(1 << 30, 32),
        name="place_mlp",
    )(w_all, *prev)


def place_up_kernel(w_ref, prev_ref, o_ref):
    o_ref[:, :FB] = w_ref[:D]
    o_ref[:, FB:] = w_ref[D:]


def place_up(l, w_all, prev):
    return pl.pallas_call(
        place_up_kernel, grid=(NDEV // 2,), in_specs=[pl.BlockSpec((2 * D, FB), lambda i: (i, 0)), ANY],
        out_specs=pl.BlockSpec((None, D, 2 * FB), lambda i: (l, 0, i)), out_shape=jax.ShapeDtypeStruct(prev.shape, BF),
        input_output_aliases={1: 0}, cost_estimate=cost(1 << 29, 16), name="place_up",
    )(w_all, prev)


def place_down_kernel(w_ref, prev_ref, o_ref):
    o_ref[...] = w_ref[...]


def place_down(l, w_all, prev):
    return pl.pallas_call(
        place_down_kernel, grid=(NDEV // 2,), in_specs=[pl.BlockSpec((D, D), lambda i: (i, 0)), ANY],
        out_specs=pl.BlockSpec((None, D, D), lambda i: (l, i, 0)), out_shape=jax.ShapeDtypeStruct(prev.shape, BF),
        input_output_aliases={1: 0}, cost_estimate=cost(1 << 29, 16), name="place_down",
    )(w_all, prev)


def place_attn_kernel(w_ref, *rest):
    o_ref = rest[-1]
    for r in range(2):
        at = slice(r * LANE, (r + 1) * LANE)
        rows = slice(r * D, (r + 1) * D)
        for k, out in enumerate(rest[-4:-1]):
            out[:, at] = w_ref[rows, k * LANE:(k + 1) * LANE]
        for c in range(D // LANE):
            o_ref[at, c * LANE:(c + 1) * LANE] = w_ref[r * D + c * LANE:r * D + (c + 1) * LANE, QKV:]


def place_attn(l, layers, w_all, prev):
    prev = list(prev)
    col = pl.BlockSpec((None, D, 2 * LANE), lambda i: (l, 0, i))
    return pl.pallas_call(
        place_attn_kernel, grid=(NDEV // 2,),
        in_specs=[pl.BlockSpec((2 * D, FB), lambda i: (i, 0))] + [ANY] * len(prev),
        out_specs=[col, col, col, pl.BlockSpec((None, 2 * LANE, D), lambda i: (l, i, 0))],
        out_shape=[jax.ShapeDtypeStruct((layers, D, D), BF)] * 4,
        input_output_aliases={1 + i: i for i in range(len(prev))},
        cost_estimate=cost(1 << 30, 16), name="place_attn",
    )(w_all, *prev)


def solution(mesh):
    act_spec = P("dp", "sp", None)
    out_four = P("dp", None, None, None)
    out_three = P("dp", None, None)

    def step(hidden_in, positions, grad_y, w_query, w_key, w_value, w_out, w_up, w_down, gain, learn_rate):
        layers = w_query.shape[0]
        idx = lax.axis_index("sp")
        chunk = SEQ // NDEV
        lr = learn_rate.reshape(1)

        def gather(t):
            return lax.all_gather(t, "sp", axis=0, tiled=True)

        def swap(t):
            return lax.all_to_all(t, "sp", 0, 0, tiled=True)

        def own(t):
            return lax.dynamic_index_in_dim(t, idx, 1, keepdims=False).reshape(SEQ, D)

        pos_tile = jnp.zeros((8, LANE), jnp.int32).at[0, :chunk].set(positions)
        pos = share(jnp.broadcast_to(pos_tile, (NDEV, 8, LANE)))[:, 0, :chunk].reshape(SEQ)

        x_all = lax.all_gather(hidden_in, "sp", axis=0, tiled=False)
        gy_all = lax.all_gather(grad_y, "sp", axis=0, tiled=False)
        lane = jnp.arange(LANE, dtype=jnp.int32)
        freqs = ROPE_BASE ** (-(lane % (HD // 2)).astype(F32) / (HD // 2))
        angles = pos.astype(F32)[:, None] * freqs[None, :]
        c_tab = jnp.cos(angles)
        s_tab = jnp.sin(angles) * jnp.where(lane % HD < HD // 2, -1.0, 1.0)[None, :]

        wq = w_query.reshape(layers, D, D)
        wk = w_key.reshape(layers, D, D)
        wv = w_value.reshape(layers, D, D)
        wo = w_out.reshape(layers, D, D)

        def gain_row(l):
            return gain[l].reshape(1, D)

        x0 = own(x_all)
        n0 = norm_apply(x0.astype(F32), gain[0]).astype(BF)
        q0, k0, v0, o0, o_pack0, lse0 = attn_fwd(0, n0, wq, wk, wv, c_tab, s_tab)
        o_all0 = swap(o_pack0)
        pre0, x1, n1 = mlp_fwd(0, False, n0, x0, o0, wo, w_up, w_down, gain_row(1))
        n1_all = gather(n1).reshape(1, NDEV, SEQ, D)
        q1, k1, v1, o1, o_pack1, lse1 = attn_fwd(1, n1, wq, wk, wv, c_tab, s_tab)
        o_all1 = swap(o_pack1)
        pre1, y = mlp_fwd(1, True, n1, x1, o1, wo, w_up, w_down, gain_row(1))
        out_y = swap(y.reshape(NDEV, chunk, D))

        gy = own(gy_all)
        dn1, d_pack1 = attn_bwd(1, gy, wo, wq, wk, wv, q1, k1, v1, lse1, c_tab, s_tab)
        d_all1 = swap(d_pack1)
        g0 = mlp_bwd(1, gy, pre1, w_up, w_down, dn1, x1, gain_row(1))
        g0_all = gather(g0).reshape(1, NDEV, SEQ, D)
        tie = lax.optimization_barrier

        dn0, d_pack0 = attn_bwd(0, g0, wo, wq, wk, wv, q0, k0, v0, lse0, c_tab, s_tab)
        d_all0 = swap(d_pack0)
        d_all1, dn0 = tie((d_all1, dn0))
        w_attn1 = dw_attn(1, lr, n1_all, gy_all, d_all1, o_all1, wq, wk, wv, wo)
        w_attn1_all = gather(w_attn1)
        dn0, w_attn1 = tie((dn0, w_attn1))
        gx = mlp_bwd(0, g0, pre0, w_up, w_down, dn0, x0, gain_row(0))
        grad_x = swap(gx.reshape(NDEV, chunk, D))
        gy_all, gx = tie((gy_all, gx))
        w_up1, w_mlp1 = dw_mlp(1, lr, n1_all, gy_all, w_up, w_down)
        w_up1_all = gather(w_up1)
        x_all, w_mlp1 = tie((x_all, w_mlp1))
        n0_all = norm_tokens(x_all.reshape(NDEV * SEQ, D), gain_row(0)).reshape(x_all.shape)
        w_attn0 = dw_attn(0, lr, n0_all, g0_all, d_all0, o_all0, wq, wk, wv, wo)
        w_attn0_all = gather(w_attn0)
        n0_all, w_attn0 = tie((n0_all, w_attn0))
        st, w_down1 = dw_chip(lr, n0_all, g0_all, w_up, w_down, w_mlp1)
        up_down = place_mlp(0, layers, st.reshape(NDEV * 2 * D, FB), (), lambda i: i)
        attn_new = place_attn(1, layers, w_attn1_all, ())
        attn_new = place_attn(0, layers, w_attn0_all, attn_new)
        new_down = place_down(1, w_down1.reshape(NDEV * FB, D), up_down[1])
        new_up = place_up(1, w_up1_all, up_down[0])
        nq, nk, nv, no = attn_new
        return (out_y, grad_x, nq.reshape(w_query.shape), nk.reshape(w_query.shape), nv.reshape(w_query.shape),
                no.reshape(w_out.shape), new_up, new_down)

    return jax.shard_map(step, mesh=mesh,
                         in_specs=(act_spec, P(("dp", "sp")), act_spec, P(), P(), P(), P(), P(), P(), P(), P()),
                         out_specs=(act_spec, act_spec, out_four, out_four, out_four, out_four, out_three, out_three),
                         check_vma=False)
```
